128 devices in a mesh: dp: 1, tp: 2 (over core), sp: 64 (over z, y, x).
Axes of the slice: x: 4, y: 4, z: 4, core: 2. Of those that a mesh axis runs over, the one named last changes fastest.
Arguments:
- hidden: bfloat16 [65536, 1024], P(('dp', 'sp'))
- w_query: bfloat16 [1024, 1024], P(None, 'tp')
- w_key: bfloat16 [1024, 1024], P(None, 'tp')
- w_value: bfloat16 [1024, 1024], P(None, 'tp')
- w_out: bfloat16 [1024, 1024], P('tp')
- branch_bias: float32 [4, 16], replicated
Outputs:
- output: bfloat16 [65536, 1024], P(('dp', 'sp'), 'tp')
All inputs are finite; a program needn't handle non-finite values.
Results may differ from the reference program's by a relative error of at most 0.00241.
Values are sent between devices in bfloat16 or wider.
A program may use at most 1 GiB of HBM per device.

```python
import jax
import jax.numpy as jnp
from jax import lax

MODEL_DIM = 1024
NUM_HEADS = 16
NUM_BRANCHES = 4
SEQ_LEN = 65536
SEG_BASE = 2048

HEAD_DIM = MODEL_DIM // NUM_HEADS
LOGIT_SCALE = HEAD_DIM ** -0.5


def setup_inputs(seed: int = 0, part: int = 0) -> dict:
    root_key = jax.random.key(seed)
    hidden_key = jax.random.fold_in(jax.random.fold_in(root_key, 1), part)
    key_list = jax.random.split(jax.random.fold_in(root_key, 2), 5)
    fan_scale = MODEL_DIM ** -0.5

    def weight(key_w, gain_factor):
        drawn = jax.random.normal(key_w, (MODEL_DIM, MODEL_DIM), jnp.float32)
        return (drawn * (gain_factor * fan_scale)).astype(jnp.bfloat16)

    hidden = jax.random.normal(hidden_key, (SEQ_LEN, MODEL_DIM), jnp.float32)
    branch_bias = jax.random.normal(key_list[4], (NUM_BRANCHES, NUM_HEADS), jnp.float32)
    return {'hidden': hidden.astype(jnp.bfloat16), 'w_query': weight(key_list[0], 1.5), 'w_key': weight(key_list[1], 1.5), 'w_value': weight(key_list[2], 1.0), 'w_out': weight(key_list[3], 2.0), 'branch_bias': branch_bias}


def attend_block(blocks):
    q_blk, k_blk, v_blk = blocks
    logits = jnp.dot(q_blk, k_blk.T, preferred_element_type=jnp.float32) * LOGIT_SCALE
    row_max = jnp.max(logits, axis=-1, keepdims=True)
    weights = jnp.exp(logits - row_max)
    row_sum = jnp.sum(weights, axis=-1, keepdims=True)
    numer_sum = jnp.dot(weights.astype(jnp.bfloat16), v_blk, preferred_element_type=jnp.float32)
    return numer_sum / row_sum, (row_max + jnp.log(row_sum))[:, 0]


def branch_attention(q_all, k_all, v_all, branch):
    dil_rate = 2 ** branch
    num_segs = SEQ_LEN // (SEG_BASE * dil_rate)
    phase_ok = jnp.arange(NUM_HEADS)[:, None] % dil_rate == jnp.arange(dil_rate)[None, :]
    phase_f = phase_ok.astype(jnp.float32)

    def pick_rows(source):
        split_rows = source.astype(jnp.float32).reshape(num_segs, SEG_BASE, dil_rate, NUM_HEADS, HEAD_DIM)
        chosen = jnp.einsum('asihd,hi->ahsd', split_rows, phase_f).astype(jnp.bfloat16)
        return chosen.reshape(num_segs * NUM_HEADS, SEG_BASE, HEAD_DIM)

    attn_out, log_norm = lax.map(attend_block, (pick_rows(q_all), pick_rows(k_all), pick_rows(v_all)))
    attn_out = attn_out.reshape(num_segs, NUM_HEADS, SEG_BASE, HEAD_DIM)
    log_norm = log_norm.reshape(num_segs, NUM_HEADS, SEG_BASE)
    out_full = jnp.einsum('ahsd,hi->asihd', attn_out, phase_f).reshape(SEQ_LEN, NUM_HEADS, HEAD_DIM)
    lse_full = jnp.einsum('ahs,hi->asih', log_norm, phase_f).reshape(SEQ_LEN, NUM_HEADS)
    mask_full = jnp.broadcast_to(phase_ok.T[None, None], (num_segs, SEG_BASE, dil_rate, NUM_HEADS)).reshape(SEQ_LEN, NUM_HEADS)
    return out_full, lse_full, mask_full


def reference(hidden, w_query, w_key, w_value, w_out, branch_bias):
    def project(weight):
        return jnp.dot(hidden, weight, preferred_element_type=jnp.float32).astype(jnp.bfloat16).reshape(SEQ_LEN, NUM_HEADS, HEAD_DIM)

    q_all = project(w_query)
    k_all = project(w_key)
    v_all = project(w_value)
    for branch in range(NUM_BRANCHES):
        out_full, lse_full, mask_full = branch_attention(q_all, k_all, v_all, branch)
        branch_score = jnp.where(mask_full, lse_full + branch_bias[branch][None, :], -jnp.inf)
        if branch == 0:
            run_num = out_full
            run_max = branch_score
            run_den = jnp.ones_like(branch_score)
        else:
            new_max = jnp.maximum(run_max, branch_score)
            keep_old = jnp.exp(run_max - new_max)
            take_new = jnp.exp(branch_score - new_max)
            run_num = run_num * keep_old[..., None] + out_full * take_new[..., None]
            run_den = run_den * keep_old + take_new
            run_max = new_max
    combined = (run_num / run_den[..., None]).astype(jnp.bfloat16).reshape(SEQ_LEN, MODEL_DIM)
    return jnp.dot(combined, w_out, preferred_element_type=jnp.float32).astype(jnp.bfloat16)
```

```python
import functools

import jax
import jax.numpy as jnp
from jax import lax
from jax.experimental import pallas as pl
from jax.experimental.pallas import tpu as pltpu
from jax.sharding import PartitionSpec as P

MESH = pl.DeviceIdType.MESH
F32 = jnp.float32
BF16 = jnp.bfloat16
ORDER = (0, 4, 2, 6, 1, 5, 3, 7)
HEADS = 8
ROWS = 1024
TILE = 256
KEYS = 2048

UNITS = (
    (0, 0, 0, 256),
    (0, 0, 256, 256),
    (2, -1, 0, 256),
    (0, 0, 512, 256),
    (0, 0, 768, 256),
    (1, 0, 0, 256),
    (1, 0, 256, 256),
    (3, -1, 0, 128),
)


def nt_dot(a, b):
    return lax.dot_general(a, b, (((1,), (1,)), ((), ())), preferred_element_type=F32)


def nn_dot(a, b):
    return jnp.dot(a, b, preferred_element_type=F32)


def kernel(hid, wq, wk, wv, wo, bias, out, hid_v, wq_v, wk_v, wv_v, wo_v, wo_x, xp, q_s, own, r1, r2, r3, r4, s0, s1, p0_s, p1_s,
           m0, m1, l0, l1, num, den, top, o_own, o_oth, outp, in_sem, ssem, rsem, osend, orecv):
    tp = lax.axis_index('tp')
    sp = lax.axis_index('sp')
    x = sp % 4
    y = (sp // 4) % 4
    peers = (sp + 1 - 2 * (x % 2), sp + 3 - 2 * x, sp + 4 * (1 - 2 * (y % 2)), sp + 4 * (3 - 2 * y))

    loads = [pltpu.make_async_copy(a, b, in_sem.at[n]) for n, (a, b) in enumerate(((hid, hid_v), (wk, wk_v), (wv, wv_v), (wq, wq_v), (wo, wo_v)))]
    for load in loads:
        load.start()

    barrier = pltpu.get_barrier_semaphore()
    for peer in peers:
        pl.semaphore_signal(barrier, inc=1, device_id={'sp': peer}, device_id_type=MESH)
    pl.semaphore_signal(barrier, inc=1, device_id={'tp': 1 - tp}, device_id_type=MESH)

    def refs(n, h):
        if n == 0:
            return own.at[h, pl.ds(0, 512)], r1.at[h, pl.ds(0, 512)], 0
        if n == 1:
            return own.at[h, pl.ds(512, 512)], r1.at[h, pl.ds(512, 512)], 0
        if n == 2:
            return own.at[h, pl.ds(0, 512)], r2.at[h, pl.ds(0, 512)], 1
        if n == 3:
            return r1.at[h, pl.ds(0, 512)], r2.at[h, pl.ds(512, 512)], 1
        if n < 8:
            src = (own.at[h, pl.ds(0, 256)], r1.at[h, pl.ds(0, 256)], r2.at[h, pl.ds(0, 256)], r2.at[h, pl.ds(512, 256)])[n - 4]
            return src, r3.at[h, pl.ds((n - 4) * 256, 256)], 2
        if n < 12:
            src = (own.at[h, pl.ds(0, 128)], r1.at[h, pl.ds(0, 128)], r2.at[h, pl.ds(0, 128)], r2.at[h, pl.ds(512, 128)])[n - 8]
        else:
            src = r3.at[h, pl.ds((n - 12) * 256, 128)]
        return src, r4.at[h, pl.ds((n - 8) * 128, 128)], 3

    def copy(n, h):
        src, dst, level = refs(n, h)
        return pltpu.make_async_remote_copy(src, dst, ssem.at[h, n], rsem.at[h, n], device_id={'sp': peers[level]}, device_id_type=MESH)

    def start(h, *chunks):
        for n in chunks:
            copy(n, h).start()

    def arrive(h, *chunks):
        for n in chunks:
            copy(n, h).wait_recv()

    def event1(h):
        arrive(h, 0)
        start(h, 3, 5, 9)
        if isinstance(h, int):
            if h + 2 < HEADS:
                start(h + 2, 2, 4, 8)
        else:
            @pl.when(h + 2 < HEADS)
            def _():
                start(h + 2, 2, 4, 8)

    def event2(h):
        arrive(h, 2)
        start(h, 6, 10)

    def event3(h):
        arrive(h, 3)
        start(h, 7, 11)

    def event4(h):
        arrive(h, 4, 5, 6, 7)
        start(h, 12, 13, 14, 15)

    row_id = lax.broadcasted_iota(jnp.int32, (128, 128), 0)
    col_id = lax.broadcasted_iota(jnp.int32, (128, 128), 1)
    gather = jnp.where(col_id == 8 * (row_id % 16) + row_id // 16, 1.0, 0.0).astype(BF16)
    spread = jnp.where(row_id == 8 * (col_id % 16) + col_id // 16, 1.0, 0.0).astype(BF16)

    loads[0].wait()
    for c in range(8):
        part = nn_dot(gather, hid_v[c * 128:(c + 1) * 128, :]).astype(BF16)
        for r in range(8):
            xp[r * 128 + c * 16:r * 128 + (c + 1) * 16, :] = part[r * 16:(r + 1) * 16, :]

    low = lax.broadcasted_iota(jnp.int32, (512, 128), 1) < 64

    def place(dst, h, half, value):
        for j in range(4):
            pos = ORDER.index((half * 4 + j - h) % 8)
            dst[h, pos * 128:(pos + 1) * 128, :] = value[j * 128:(j + 1) * 128, :]

    loads[1].wait()
    loads[2].wait()
    for half in range(2):
        rows = xp[half * 512:(half + 1) * 512, :]
        key = nn_dot(rows, wk_v[...])
        val = nn_dot(rows, wv_v[...])
        for a in range(4):
            kp = key[:, a * 128:(a + 1) * 128]
            vp = pltpu.roll(val[:, a * 128:(a + 1) * 128], 64, 1)
            place(own, 2 * a, half, jnp.where(low, kp, vp).astype(BF16))
            place(own, 2 * a + 1, half, jnp.where(low, vp, kp).astype(BF16))

    pl.semaphore_wait(barrier, 5)
    for h in range(HEADS):
        start(h, 0, 1)
    for h in range(2):
        start(h, 2, 4, 8)
    loads[4].wait()
    send_w = pltpu.make_async_remote_copy(
        wo_v.at[:, pl.ds(pl.multiple_of((1 - tp) * 512, 512), 512)], wo_x, osend.at[4], orecv.at[4],
        device_id={'tp': 1 - tp}, device_id_type=MESH)
    send_w.start()

    loads[3].wait()
    for half in range(2):
        qry = nn_dot(xp[half * 512:(half + 1) * 512, :], wq_v[...]) * 0.125
        for a in range(4):
            qp = qry[:, a * 128:(a + 1) * 128]
            place(q_s, 2 * a, half, jnp.where(low, qp, 0.0).astype(BF16))
            place(q_s, 2 * a + 1, half, jnp.where(low, 0.0, qp).astype(BF16))
    o_own[...] = jnp.zeros_like(o_own)

    def keys(branch, h):
        if branch == 0:
            parts = [own[h], r1[h]]
        elif branch == 1:
            parts = [own[h, 0:512, :], r1[h, 0:512, :], r2[h]]
        elif branch == 2:
            parts = [own[h, 0:256, :], r1[h, 0:256, :], r2[h, 0:256, :], r2[h, 512:768, :], r3[h]]
        else:
            parts = [own[h, 0:128, :], r1[h, 0:128, :], r2[h, 0:128, :], r2[h, 512:640, :]]
            parts += [r3[h, c * 256:c * 256 + 128, :] for c in range(4)] + [r4[h]]
        return jnp.concatenate(parts, axis=0)

    def logits(u, h):
        branch, shift, first, rows = UNITS[u]
        h = h + shift
        dst = (s0, s1)[u % 2]
        dst[0:rows, :] = nt_dot(q_s[h, first:first + rows, :], keys(branch, h))

    def soften(u):
        rows = UNITS[u][3]
        src, dst, mx, sm = (s0, s1)[u % 2], (p0_s, p1_s)[u % 2], (m0, m1)[u % 2], (l0, l1)[u % 2]
        for g in range(rows // 16):
            at = slice(g * 16, (g + 1) * 16)
            s = src[at, :]
            m = jnp.max(s, axis=1, keepdims=True)
            e = jnp.exp(s - m)
            dst[at, :] = e.astype(BF16)
            mx[at, :] = jnp.broadcast_to(m, (16, 128))
            sm[at, :] = jnp.broadcast_to(jnp.sum(e, axis=1, keepdims=True), (16, 128))

    def gain(u, h):
        branch, shift, first, rows = UNITS[u]
        h = h + shift
        src, mx, sm = (p0_s, p1_s)[u % 2], (m0, m1)[u % 2], (l0, l1)[u % 2]
        got = nn_dot(src[0:rows, :], keys(branch, h))
        slot = h % 2
        at = slice(first, first + rows)
        score = mx[0:rows, :] + bias[branch, tp * HEADS + h]
        if branch == 0:
            num[slot, at, :] = got
            den[slot, at, :] = sm[0:rows, :]
            top[slot, at, :] = score
        else:
            old = top[slot, at, :]
            new = jnp.maximum(old, score)
            keep = jnp.exp(old - new)
            take = jnp.exp(score - new)
            num[slot, at, :] = num[slot, at, :] * keep + got * take
            den[slot, at, :] = den[slot, at, :] * keep + sm[0:rows, :] * take
            top[slot, at, :] = new

    lane = lax.broadcasted_iota(jnp.int32, (128, 128), 1)

    def send_o(a):
        return pltpu.make_async_remote_copy(o_own.at[a], o_oth.at[a], osend.at[a], orecv.at[a], device_id={'tp': 1 - tp}, device_id_type=MESH)

    def finish(h):
        a = h // 2
        limit = 128 - 64 * (h % 2)
        for pos in range(8):
            at = pl.ds(pl.multiple_of(((ORDER[pos] + h) % 8) * 128, 128), 128)
            got = num[h % 2, pos * 128:(pos + 1) * 128, :] / den[h % 2, pos * 128:(pos + 1) * 128, :]
            o_own[a, at, :] = jnp.where(lane < limit, got, o_own[a, at, :].astype(F32)).astype(BF16)
        if isinstance(h, int):
            if h % 2 == 1:
                send_o(a).start()
        else:
            @pl.when(h % 2 == 1)
            def _():
                send_o(a).start()

    event1(0)
    event2(0)

    first = [u for u in range(8) if UNITS[u][1] == 0]

    def before(u, h):
        if u == 0:
            arrive(h, 1)
        elif u == 2:
            event4(h - 1)
        elif u == 3:
            event3(h)
        elif u == 5:
            if isinstance(h, int):
                if h + 1 < HEADS:
                    event1(h + 1)
                    event2(h + 1)
            else:
                @pl.when(h + 1 < HEADS)
                def _():
                    event1(h + 1)
                    event2(h + 1)
        elif u == 7:
            arrive(h - 1, *range(8, 16))

    queue = []
    for u in (0, 1):
        before(u, 0)
        logits(u, 0)
        if u == 1:
            soften(0)
    before(3, 0)
    gain(0, 0)
    soften(1)
    gain(1, 0)
    for u in (4, 3):
        logits(u, 0)
    soften(4)
    soften(3)
    gain(4, 0)
    gain(3, 0)
    before(5, 0)
    logits(5, 0)
    logits(6, 0)
    soften(5)
    gain(5, 0)
    soften(6)

    def step(h, carry):
        for u in range(8):
            before(u, h)
            logits(u, h)
            if u == 0:
                gain(6, h - 1)
            else:
                soften(u - 1)
                if u >= 2:
                    gain(u - 2, h)
        soften(7)
        gain(6, h)
        gain(7, h)
        finish(h - 1)
        return carry

    def run(h, carry):
        return step(h, carry)

    def whole(h, carry):
        for u in range(8):
            before(u, h)
            logits(u, h)
            if u >= 1:
                soften(u - 1)
            if u >= 2:
                gain(u - 2, h)
        soften(7)
        gain(6, h)
        gain(7, h)
        finish(h - 1)
        return carry

    gain(6, 0)
    lax.fori_loop(1, HEADS, whole, 0)

    before(2, HEADS)
    logits(2, HEADS)
    soften(2)
    before(7, HEADS)
    logits(7, HEADS)
    gain(2, HEADS)
    soften(7)
    gain(7, HEADS)
    finish(HEADS - 1)

    send_w.wait()
    for a in range(4):
        send_o(a).wait()
    mine = pl.ds(pl.multiple_of(tp * 512, 512), 512)

    def swapped(ref, cols):
        parts = []
        for a in range(4):
            parts += [ref[a * 128 + 64:a * 128 + 128, cols], ref[a * 128:a * 128 + 64, cols]]
        return parts

    w_all = jnp.concatenate(swapped(wo_v, mine) + swapped(wo_x, slice(None)), axis=0)
    for half in range(2):
        at = slice(half * 512, (half + 1) * 512)
        o_all = jnp.concatenate([o_own[a, at, :] for a in range(4)] + [o_oth[a, at, :] for a in range(4)], axis=1)
        outp[at, :] = nn_dot(o_all, w_all).astype(BF16)
    for c in range(8):
        part = jnp.concatenate([outp[r * 128 + c * 16:r * 128 + (c + 1) * 16, :] for r in range(8)], axis=0)
        out[c * 128:(c + 1) * 128, :] = nn_dot(spread, part).astype(BF16)

    def drain(h, carry):
        for n in range(16):
            copy(n, h).wait_send()
        return carry

    lax.fori_loop(0, HEADS, drain, 0)


def solution(mesh):
    def device_fn(hidden, w_query, w_key, w_value, w_out, branch_bias):
        kv = pltpu.VMEM((HEADS, ROWS, 128), BF16)
        return pl.pallas_call(
            kernel,
            out_shape=jax.ShapeDtypeStruct((ROWS, 512), BF16),
            in_specs=[pl.BlockSpec(memory_space=pl.ANY)] * 5 + [pl.BlockSpec(memory_space=pltpu.SMEM)],
            out_specs=pl.BlockSpec(memory_space=pltpu.VMEM),
            scratch_shapes=[
                pltpu.VMEM((ROWS, 1024), BF16),
                pltpu.VMEM((1024, 512), BF16), pltpu.VMEM((1024, 512), BF16), pltpu.VMEM((1024, 512), BF16),
                pltpu.VMEM((512, 1024), BF16), pltpu.VMEM((512, 512), BF16),
                pltpu.VMEM((ROWS, 1024), BF16),
                kv, kv, kv, kv, kv, kv,
                pltpu.VMEM((TILE, KEYS), F32), pltpu.VMEM((TILE, KEYS), F32),
                pltpu.VMEM((TILE, KEYS), BF16), pltpu.VMEM((TILE, KEYS), BF16),
                pltpu.VMEM((TILE, 128), F32), pltpu.VMEM((TILE, 128), F32),
                pltpu.VMEM((TILE, 128), F32), pltpu.VMEM((TILE, 128), F32),
                pltpu.VMEM((2, ROWS, 128), F32), pltpu.VMEM((2, ROWS, 128), F32), pltpu.VMEM((2, ROWS, 128), F32),
                pltpu.VMEM((4, ROWS, 128), BF16), pltpu.VMEM((4, ROWS, 128), BF16),
                pltpu.VMEM((ROWS, 512), BF16),
                pltpu.SemaphoreType.DMA((5,)),
                pltpu.SemaphoreType.DMA((HEADS, 16)), pltpu.SemaphoreType.DMA((HEADS, 16)),
                pltpu.SemaphoreType.DMA((5,)), pltpu.SemaphoreType.DMA((5,)),
            ],
            compiler_params=pltpu.CompilerParams(collective_id=0, has_side_effects=True, vmem_limit_bytes=62 * 1024 * 1024),
            name='dilated',
        )(hidden, w_query, w_key, w_value, w_out, branch_bias)

    return jax.shard_map(device_fn, mesh=mesh, in_specs=(P(('dp', 'sp'), None), P(None, 'tp'), P(None, 'tp'), P(None, 'tp'), P('tp', None), P(None, None)), out_specs=P(('dp', 'sp'), 'tp'), check_vma=False)
```

```python
import functools

import jax
import jax.numpy as jnp
from jax import lax
from jax.experimental import pallas as pl
from jax.experimental.pallas import tpu as pltpu
from jax.sharding import PartitionSpec as P

MESH = pl.DeviceIdType.MESH
F32 = jnp.float32
BF16 = jnp.bfloat16
ORDER = (0, 4, 2, 6, 1, 5, 3, 7)
HEADS = 8
ROWS = 1024
TILE = 256
KEYS = 2048

UNITS = (
    (0, 0, 0, 256),
    (0, 0, 256, 256),
    (0, 0, 512, 256),
    (0, 0, 768, 256),
    (2, -1, 0, 256),
    (1, 0, 0, 256),
    (1, 0, 256, 256),
    (3, -2, 0, 128),
)


def nt_dot(a, b):
    return lax.dot_general(a, b, (((1,), (1,)), ((), ())), preferred_element_type=F32)


def nn_dot(a, b):
    return jnp.dot(a, b, preferred_element_type=F32)


def kernel(hid, wq, wk, wv, wo, bias, out, hid_v, wq_v, wk_v, wv_v, wo_v, wo_x, xp, q_s, own, r1, r2, r3, r4, s0, s1, p0_s, p1_s,
           m0, m1, l0, l1, num, den, top, o_own, o_oth, outp, in_sem, ssem, rsem, osend, orecv):
    tp = lax.axis_index('tp')
    sp = lax.axis_index('sp')
    x = sp % 4
    y = (sp // 4) % 4
    peers = (sp + 1 - 2 * (x % 2), sp + 3 - 2 * x, sp + 4 * (1 - 2 * (y % 2)), sp + 4 * (3 - 2 * y))

    loads = [pltpu.make_async_copy(a, b, in_sem.at[n]) for n, (a, b) in enumerate(((hid, hid_v), (wk, wk_v), (wv, wv_v), (wq, wq_v), (wo, wo_v)))]
    for load in loads:
        load.start()

    barrier = pltpu.get_barrier_semaphore()
    for peer in peers:
        pl.semaphore_signal(barrier, inc=1, device_id={'sp': peer}, device_id_type=MESH)
    pl.semaphore_signal(barrier, inc=1, device_id={'tp': 1 - tp}, device_id_type=MESH)

    def refs(n, h):
        if n == 0:
            return own.at[h, pl.ds(0, 512)], r1.at[h, pl.ds(0, 512)], 0
        if n == 1:
            return own.at[h, pl.ds(512, 512)], r1.at[h, pl.ds(512, 512)], 0
        if n == 2:
            return own.at[h, pl.ds(0, 512)], r2.at[h, pl.ds(0, 512)], 1
        if n == 3:
            return r1.at[h, pl.ds(0, 512)], r2.at[h, pl.ds(512, 512)], 1
        if n < 8:
            src = (own.at[h, pl.ds(0, 256)], r1.at[h, pl.ds(0, 256)], r2.at[h, pl.ds(0, 256)], r2.at[h, pl.ds(512, 256)])[n - 4]
            return src, r3.at[h, pl.ds((n - 4) * 256, 256)], 2
        if n < 12:
            src = (own.at[h, pl.ds(0, 128)], r1.at[h, pl.ds(0, 128)], r2.at[h, pl.ds(0, 128)], r2.at[h, pl.ds(512, 128)])[n - 8]
        else:
            src = r3.at[h, pl.ds((n - 12) * 256, 128)]
        return src, r4.at[h, pl.ds((n - 8) * 128, 128)], 3

    def copy(n, h):
        src, dst, level = refs(n, h)
        sem = n if n < 4 else level + 2
        return pltpu.make_async_remote_copy(src, dst, ssem.at[level], rsem.at[h, sem], device_id={'sp': peers[level]}, device_id_type=MESH)

    def start(h, *chunks):
        for n in chunks:
            copy(n, h).start()

    def arrive(h, n):
        copy(n, h).wait_recv()

    def arrive_all(h, level):
        dst = (r3, r4)[level - 2].at[h]
        pltpu.make_async_remote_copy(dst, dst, ssem.at[level], rsem.at[h, level + 2], device_id={'sp': peers[level]}, device_id_type=MESH).wait_recv()

    def sent(level):
        pltpu.make_async_remote_copy(own, own, ssem.at[level], rsem.at[0, 0], device_id={'sp': peers[level]}, device_id_type=MESH).wait_send()

    def event1(h):
        arrive(h, 0)
        start(h, 3, 5, 9)
        if isinstance(h, int):
            if h + 2 < HEADS:
                start(h + 2, 2, 4, 8)
        else:
            @pl.when(h + 2 < HEADS)
            def _():
                start(h + 2, 2, 4, 8)

    def event2(h):
        arrive(h, 2)
        start(h, 6, 10)

    def event3(h):
        arrive(h, 3)
        start(h, 7, 11)

    def event4(h):
        arrive_all(h, 2)
        start(h, 12, 13, 14, 15)

    row_id = lax.broadcasted_iota(jnp.int32, (128, 128), 0)
    col_id = lax.broadcasted_iota(jnp.int32, (128, 128), 1)
    gather = jnp.where(col_id == 8 * (row_id % 16) + row_id // 16, 1.0, 0.0).astype(BF16)
    spread = jnp.where(row_id == 8 * (col_id % 16) + col_id // 16, 1.0, 0.0).astype(BF16)

    loads[0].wait()
    for c in range(8):
        part = nn_dot(gather, hid_v[c * 128:(c + 1) * 128, :]).astype(BF16)
        for r in range(8):
            xp[r * 128 + c * 16:r * 128 + (c + 1) * 16, :] = part[r * 16:(r + 1) * 16, :]

    low = lax.broadcasted_iota(jnp.int32, (512, 128), 1) < 64

    def place(dst, h, half, value):
        for j in range(4):
            pos = ORDER.index((half * 4 + j - h) % 8)
            dst[h, pos * 128:(pos + 1) * 128, :] = value[j * 128:(j + 1) * 128, :]

    def project_kv(cols):
        for half in range(2):
            rows = xp[half * 512:(half + 1) * 512, :]
            key = nn_dot(rows, wk_v[:, cols * 256:(cols + 1) * 256])
            val = nn_dot(rows, wv_v[:, cols * 256:(cols + 1) * 256])
            for a in range(2):
                h = 4 * cols + 2 * a
                kp = key[:, a * 128:(a + 1) * 128]
                vp = pltpu.roll(val[:, a * 128:(a + 1) * 128], 64, 1)
                place(own, h, half, jnp.where(low, kp, vp).astype(BF16))
                place(own, h + 1, half, jnp.where(low, vp, kp).astype(BF16))

    def project_q(cols):
        for half in range(2):
            qry = nn_dot(xp[half * 512:(half + 1) * 512, :], wq_v[:, cols * 256:(cols + 1) * 256]) * 0.125
            for a in range(2):
                h = 4 * cols + 2 * a
                qp = qry[:, a * 128:(a + 1) * 128]
                place(q_s, h, half, jnp.where(low, qp, 0.0).astype(BF16))
                place(q_s, h + 1, half, jnp.where(low, 0.0, qp).astype(BF16))

    loads[1].wait()
    loads[2].wait()
    project_kv(0)
    pl.semaphore_wait(barrier, 5)
    for h in range(2):
        start(h, 0, 1, 2, 4, 8)
    for h in range(2, 4):
        start(h, 0, 1)
    project_kv(1)
    for h in range(4, HEADS):
        start(h, 0, 1)
    loads[4].wait()
    send_w = pltpu.make_async_remote_copy(
        wo_v.at[:, pl.ds(pl.multiple_of((1 - tp) * 512, 512), 512)], wo_x, osend.at[4], orecv.at[4],
        device_id={'tp': 1 - tp}, device_id_type=MESH)
    send_w.start()
    loads[3].wait()
    project_q(0)
    project_q(1)
    o_own[...] = jnp.zeros_like(o_own)

    def keys(branch, h):
        if branch == 0:
            parts = [own[h], r1[h]]
        elif branch == 1:
            parts = [own[h, 0:512, :], r1[h, 0:512, :], r2[h]]
        elif branch == 2:
            parts = [own[h, 0:256, :], r1[h, 0:256, :], r2[h, 0:256, :], r2[h, 512:768, :], r3[h]]
        else:
            parts = [own[h, 0:128, :], r1[h, 0:128, :], r2[h, 0:128, :], r2[h, 512:640, :]]
            parts += [r3[h, c * 256:c * 256 + 128, :] for c in range(4)] + [r4[h]]
        return jnp.concatenate(parts, axis=0)

    def logits(unit, slot):
        branch, h, first, rows = unit
        (s0, s1)[slot][0:rows, :] = nt_dot(q_s[h, first:first + rows, :], keys(branch, h))

    def soften(unit, slot):
        src, dst, mx, sm = (s0, s1)[slot], (p0_s, p1_s)[slot], (m0, m1)[slot], (l0, l1)[slot]
        for g in range(unit[3] // 16):
            at = slice(g * 16, (g + 1) * 16)
            s = src[at, :]
            m = jnp.max(s, axis=1, keepdims=True)
            e = jnp.exp(s - m)
            dst[at, :] = e.astype(BF16)
            mx[at, :] = jnp.broadcast_to(m, (16, 128))
            sm[at, :] = jnp.broadcast_to(jnp.sum(e, axis=1, keepdims=True), (16, 128))

    def gain(unit, slot):
        branch, h, first, rows = unit
        src, mx, sm = (p0_s, p1_s)[slot], (m0, m1)[slot], (l0, l1)[slot]
        got = nn_dot(src[0:rows, :], keys(branch, h))
        at = slice(first, first + rows)
        score = mx[0:rows, :] + bias[branch, tp * HEADS + h]
        if branch == 0:
            num[h, at, :] = got
            den[h, at, :] = sm[0:rows, :]
            top[h, at, :] = score
        else:
            old = top[h, at, :]
            new = jnp.maximum(old, score)
            keep = jnp.exp(old - new)
            take = jnp.exp(score - new)
            num[h, at, :] = num[h, at, :] * keep + got * take
            den[h, at, :] = den[h, at, :] * keep + sm[0:rows, :] * take
            top[h, at, :] = new

    lane = lax.broadcasted_iota(jnp.int32, (128, 128), 1)

    def send_o(a):
        return pltpu.make_async_remote_copy(o_own.at[a], o_oth.at[a], osend.at[a], orecv.at[a], device_id={'tp': 1 - tp}, device_id_type=MESH)

    def finish(h):
        a = h // 2
        limit = 128 - 64 * (h % 2)
        for pos in range(8):
            at = pl.ds(pl.multiple_of(((ORDER[pos] + h) % 8) * 128, 128), 128)
            got = num[h, pos * 128:(pos + 1) * 128, :] / den[h, pos * 128:(pos + 1) * 128, :]
            o_own[a, at, :] = jnp.where(lane < limit, got, o_own[a, at, :].astype(F32)).astype(BF16)

    def unit_of(u, h):
        branch, shift, first, rows = UNITS[u]
        return branch, h + shift, first, rows

    def push(flight, unit):
        slot = flight[-1][1] ^ 1 if flight else 0
        logits(unit, slot)
        if flight:
            soften(*flight[-1])
        done = None
        if len(flight) == 2:
            gain(*flight[0])
            done = flight[0][0]
            flight = flight[1:]
        return flight + [(unit, slot)], done

    def run(flight, units):
        for unit in units:
            flight, done = push(flight, unit)
            if done is not None and done[0] == 3:
                finish(done[1])
        return flight

    event1(0)
    event2(0)
    arrive(0, 1)
    event3(0)
    event1(1)
    event2(1)
    flight = run([], [unit_of(u, 0) for u in (0, 1, 2, 3, 5, 6)])
    arrive(1, 1)
    event4(0)
    event3(1)
    event1(2)
    event2(2)
    flight = run(flight, [unit_of(u, 1) for u in range(7)])

    def body(h, carry):
        arrive(h, 1)
        event4(h - 1)
        event3(h)

        @pl.when(h + 1 < HEADS)
        def _():
            event1(h + 1)
            event2(h + 1)

        @pl.when((h >= 4) & (h % 2 == 0))
        def _():
            send_o((h - 4) // 2).start()

        arrive_all(h - 2, 3)
        units = [unit_of(7, h)] + [unit_of(u, h) for u in range(7)]
        into = [(unit_of(5, h - 1), flight[0][1]), (unit_of(6, h - 1), flight[1][1])]
        left = run(into, units)
        assert [f[1] for f in left] == [f[1] for f in flight]
        return carry

    lax.fori_loop(2, HEADS, body, 0)
    flight = [(unit_of(5, HEADS - 1), flight[0][1]), (unit_of(6, HEADS - 1), flight[1][1])]
    event4(HEADS - 1)
    send_o(2).start()
    arrive_all(HEADS - 2, 3)
    flight = run(flight, [unit_of(7, HEADS), unit_of(4, HEADS)])
    arrive_all(HEADS - 1, 3)
    flight = run(flight, [unit_of(7, HEADS + 1)])
    soften(*flight[1])
    gain(*flight[0])
    gain(*flight[1])
    finish(HEADS - 1)
    send_o(3).start()

    send_w.wait()
    for a in range(4):
        send_o(a).wait()
    mine = pl.ds(pl.multiple_of(tp * 512, 512), 512)

    def swapped(ref, cols):
        parts = []
        for a in range(4):
            parts += [ref[a * 128 + 64:a * 128 + 128, cols], ref[a * 128:a * 128 + 64, cols]]
        return parts

    w_all = jnp.concatenate(swapped(wo_v, mine) + swapped(wo_x, slice(None)), axis=0)
    for half in range(2):
        at = slice(half * 512, (half + 1) * 512)
        o_all = jnp.concatenate([o_own[a, at, :] for a in range(4)] + [o_oth[a, at, :] for a in range(4)], axis=1)
        outp[at, :] = nn_dot(o_all, w_all).astype(BF16)
    for c in range(8):
        part = jnp.concatenate([outp[r * 128 + c * 16:r * 128 + (c + 1) * 16, :] for r in range(8)], axis=0)
        out[c * 128:(c + 1) * 128, :] = nn_dot(spread, part).astype(BF16)

    for level in range(4):
        sent(level)


def solution(mesh):
    def device_fn(hidden, w_query, w_key, w_value, w_out, branch_bias):
        kv = pltpu.VMEM((HEADS, ROWS, 128), BF16)
        return pl.pallas_call(
            kernel,
            out_shape=jax.ShapeDtypeStruct((ROWS, 512), BF16),
            in_specs=[pl.BlockSpec(memory_space=pl.ANY)] * 5 + [pl.BlockSpec(memory_space=pltpu.SMEM)],
            out_specs=pl.BlockSpec(memory_space=pltpu.VMEM),
            scratch_shapes=[
                pltpu.VMEM((ROWS, 1024), BF16),
                pltpu.VMEM((1024, 512), BF16), pltpu.VMEM((1024, 512), BF16), pltpu.VMEM((1024, 512), BF16),
                pltpu.VMEM((512, 1024), BF16), pltpu.VMEM((512, 512), BF16),
                pltpu.VMEM((ROWS, 1024), BF16),
                kv, kv, kv, kv, kv, kv,
                pltpu.VMEM((TILE, KEYS), F32), pltpu.VMEM((TILE, KEYS), F32),
                pltpu.VMEM((TILE, KEYS), BF16), pltpu.VMEM((TILE, KEYS), BF16),
                pltpu.VMEM((TILE, 128), F32), pltpu.VMEM((TILE, 128), F32),
                pltpu.VMEM((TILE, 128), F32), pltpu.VMEM((TILE, 128), F32),
                pltpu.VMEM((HEADS, ROWS, 128), F32), pltpu.VMEM((HEADS, ROWS, 128), F32), pltpu.VMEM((HEADS, ROWS, 128), F32),
                pltpu.VMEM((4, ROWS, 128), BF16), pltpu.VMEM((4, ROWS, 128), BF16),
                pltpu.VMEM((ROWS, 512), BF16),
                pltpu.SemaphoreType.DMA((5,)),
                pltpu.SemaphoreType.DMA((4,)), pltpu.SemaphoreType.DMA((HEADS, 6)),
                pltpu.SemaphoreType.DMA((5,)), pltpu.SemaphoreType.DMA((5,)),
            ],
            compiler_params=pltpu.CompilerParams(collective_id=0, has_side_effects=True, vmem_limit_bytes=62 * 1024 * 1024),
            name='dilated',
        )(hidden, w_query, w_key, w_value, w_out, branch_bias)

    return jax.shard_map(device_fn, mesh=mesh, in_specs=(P(('dp', 'sp'), None), P(None, 'tp'), P(None, 'tp'), P(None, 'tp'), P('tp', None), P(None, None)), out_specs=P(('dp', 'sp'), 'tp'), check_vma=False)
```

```python
import functools

import jax
import jax.numpy as jnp
from jax import lax
from jax.experimental import pallas as pl
from jax.experimental.pallas import tpu as pltpu
from jax.sharding import PartitionSpec as P

MESH = pl.DeviceIdType.MESH
F32 = jnp.float32
BF16 = jnp.bfloat16
ORDER = (0, 4, 2, 6, 1, 5, 3, 7)
HEADS = 8
ROWS = 1024
TILE = 256
LANE = 128
HALF = 512
DIM = 64
KEYS = 2048
SLOTS = 2

UNITS = (
    (0, 0, 0, 256),
    (0, 0, 256, 256),
    (0, 0, 512, 256),
    (0, 0, 768, 256),
    (2, -1, 0, 256),
    (1, 0, 0, 256),
    (1, 0, 256, 256),
    (3, -2, 0, 128),
)


def nt_dot(a, b):
    return lax.dot_general(a, b, (((1,), (1,)), ((), ())), preferred_element_type=F32)


def nn_dot(a, b):
    return jnp.dot(a, b, preferred_element_type=F32)


def kernel(hid, wq, wk, wv, wo, bias, out, hid_v, wq_v, wk_v, wv_v, wo_v, wo_x, xp, q_s, own, r1, r2, r3, r4, *more):
    S, PR, M, L = (more[n * SLOTS:(n + 1) * SLOTS] for n in range(4))
    num, den, top, o_own, o_oth, part_o, in_sem, ssem, rsem, osend, orecv = more[4 * SLOTS:]
    tp = lax.axis_index('tp')
    sp = lax.axis_index('sp')
    x = sp % 4
    y = (sp // 4) % 4
    peers = (sp + 1 - 2 * (x % 2), sp + 3 - 2 * x, sp + 4 * (1 - 2 * (y % 2)), sp + 4 * (3 - 2 * y))

    loads = [pltpu.make_async_copy(a, b, in_sem.at[n]) for n, (a, b) in enumerate(((hid, hid_v), (wk, wk_v), (wv, wv_v), (wq, wq_v), (wo, wo_v)))]
    for load in loads:
        load.start()

    barrier = pltpu.get_barrier_semaphore()
    for peer in peers:
        pl.semaphore_signal(barrier, inc=1, device_id={'sp': peer}, device_id_type=MESH)
    pl.semaphore_signal(barrier, inc=1, device_id={'tp': 1 - tp}, device_id_type=MESH)

    def refs(n, h):
        if n == 0:
            return own.at[h, pl.ds(0, HALF)], r1.at[h, pl.ds(0, HALF)], 0
        if n == 1:
            return own.at[h, pl.ds(HALF, HALF)], r1.at[h, pl.ds(HALF, HALF)], 0
        if n == 2:
            return own.at[h, pl.ds(0, HALF)], r2.at[h, pl.ds(0, HALF)], 1
        if n == 3:
            return r1.at[h, pl.ds(0, HALF)], r2.at[h, pl.ds(HALF, HALF)], 1
        if n < 8:
            src = (own.at[h, pl.ds(0, TILE)], r1.at[h, pl.ds(0, TILE)], r2.at[h, pl.ds(0, TILE)], r2.at[h, pl.ds(HALF, TILE)])[n - 4]
            return src, r3.at[h, pl.ds((n - 4) * TILE, TILE)], 2
        if n < 12:
            src = (own.at[h, pl.ds(0, LANE)], r1.at[h, pl.ds(0, LANE)], r2.at[h, pl.ds(0, LANE)], r2.at[h, pl.ds(HALF, LANE)])[n - 8]
        else:
            src = r3.at[h, pl.ds((n - 12) * TILE, LANE)]
        return src, r4.at[h, pl.ds((n - 8) * LANE, LANE)], 3

    def copy(n, h):
        src, dst, level = refs(n, h)
        sem = n if n < 4 else level + 2
        return pltpu.make_async_remote_copy(src, dst, ssem.at[level], rsem.at[h, sem], device_id={'sp': peers[level]}, device_id_type=MESH)

    def start(h, *chunks):
        for n in chunks:
            copy(n, h).start()

    def arrive(h, n):
        copy(n, h).wait_recv()

    def arrive_all(h, level):
        dst = (r3, r4)[level - 2].at[h]
        pltpu.make_async_remote_copy(dst, dst, ssem.at[level], rsem.at[h, level + 2], device_id={'sp': peers[level]}, device_id_type=MESH).wait_recv()

    def sent(level):
        pltpu.make_async_remote_copy(own, own, ssem.at[level], rsem.at[0, 0], device_id={'sp': peers[level]}, device_id_type=MESH).wait_send()

    def event1(h):
        arrive(h, 0)
        start(h, 3, 5, 9)
        if isinstance(h, int):
            if h + 2 < HEADS:
                start(h + 2, 2, 4, 8)
        else:
            @pl.when(h + 2 < HEADS)
            def _():
                start(h + 2, 2, 4, 8)

    def event2(h):
        arrive(h, 2)
        start(h, 6, 10)

    def event3(h):
        arrive(h, 3)
        start(h, 7, 11)

    def event4(h):
        arrive_all(h, 2)
        start(h, 12, 13, 14, 15)

    row_id = lax.broadcasted_iota(jnp.int32, (LANE, LANE), 0)
    col_id = lax.broadcasted_iota(jnp.int32, (LANE, LANE), 1)
    gather = jnp.where(col_id == 8 * (row_id % 16) + row_id // 16, 1.0, 0.0).astype(BF16)

    loads[0].wait()
    for c in range(8):
        part = nn_dot(gather, hid_v[c * LANE:(c + 1) * LANE, :]).astype(BF16)
        for r in range(8):
            xp[r * LANE + c * 16:r * LANE + (c + 1) * 16, :] = part[r * 16:(r + 1) * 16, :]

    low = lax.broadcasted_iota(jnp.int32, (HALF, LANE), 1) < DIM

    def place(dst, h, half, value):
        for j in range(4):
            pos = ORDER.index((half * 4 + j - h) % 8)
            dst[h, pos * LANE:(pos + 1) * LANE, :] = value[j * LANE:(j + 1) * LANE, :]

    def project_kv(cols):
        for half in range(2):
            rows = xp[half * HALF:(half + 1) * HALF, :]
            key = nn_dot(rows, wk_v[:, cols * TILE:(cols + 1) * TILE])
            val = nn_dot(rows, wv_v[:, cols * TILE:(cols + 1) * TILE])
            for a in range(2):
                h = 4 * cols + 2 * a
                kp = key[:, a * LANE:(a + 1) * LANE]
                vp = pltpu.roll(val[:, a * LANE:(a + 1) * LANE], DIM, 1)
                place(own, h, half, jnp.where(low, kp, vp).astype(BF16))
                place(own, h + 1, half, jnp.where(low, vp, kp).astype(BF16))

    def project_q(cols):
        for half in range(2):
            qry = nn_dot(xp[half * HALF:(half + 1) * HALF, :], wq_v[:, cols * TILE:(cols + 1) * TILE]) * 0.125
            for a in range(2):
                h = 4 * cols + 2 * a
                qp = qry[:, a * LANE:(a + 1) * LANE]
                place(q_s, h, half, jnp.where(low, qp, 0.0).astype(BF16))
                place(q_s, h + 1, half, jnp.where(low, 0.0, qp).astype(BF16))

    loads[1].wait()
    loads[2].wait()
    project_kv(0)
    pl.semaphore_wait(barrier, 5)
    for h in range(2):
        start(h, 0, 1, 2, 4, 8)
    for h in range(2, 4):
        start(h, 0, 1)
    project_kv(1)
    for h in range(4, HEADS):
        start(h, 0, 1)
    loads[4].wait()
    send_w = pltpu.make_async_remote_copy(
        wo_v.at[:, pl.ds(pl.multiple_of((1 - tp) * HALF, HALF), HALF)], wo_x, osend.at[4], orecv.at[4],
        device_id={'tp': 1 - tp}, device_id_type=MESH)
    send_w.start()
    loads[3].wait()
    project_q(0)
    project_q(1)
    o_own[...] = jnp.zeros_like(o_own)

    def keys(branch, h):
        if branch == 0:
            parts = [own[h], r1[h]]
        elif branch == 1:
            parts = [own[h, 0:HALF, :], r1[h, 0:HALF, :], r2[h]]
        elif branch == 2:
            parts = [own[h, 0:TILE, :], r1[h, 0:TILE, :], r2[h, 0:TILE, :], r2[h, HALF:768, :], r3[h]]
        else:
            parts = [own[h, 0:LANE, :], r1[h, 0:LANE, :], r2[h, 0:LANE, :], r2[h, HALF:640, :]]
            parts += [r3[h, c * TILE:c * TILE + LANE, :] for c in range(4)] + [r4[h]]
        return jnp.concatenate(parts, axis=0)

    def logits(unit, slot):
        branch, h, first, rows = unit
        s = nt_dot(q_s[h, first:first + rows, :], keys(branch, h))
        S[slot][0:rows, :] = s
        L[slot][0:rows, :] = functools.reduce(jnp.maximum, [s[:, c * LANE:(c + 1) * LANE] for c in range(16)])

    def soften(unit, slot):
        rows = unit[3]
        m = jnp.max(L[slot][0:rows, :], axis=1, keepdims=True)
        e = jnp.exp(S[slot][0:rows, :] - m)
        PR[slot][0:rows, :] = e.astype(BF16)
        M[slot][0:rows, :] = jnp.broadcast_to(m, (rows, LANE))
        L[slot][0:rows, :] = jnp.broadcast_to(jnp.sum(e, axis=1, keepdims=True), (rows, LANE))

    def gain(unit, slot):
        branch, h, first, rows = unit
        src, mx = PR[slot], M[slot]
        sm = L[slot][0:rows, :]
        got = nn_dot(src[0:rows, :], keys(branch, h))
        at = slice(first, first + rows)
        score = mx[0:rows, :] + bias[branch, tp * HEADS + h]
        if branch == 0:
            num[h % 4, at, :] = got
            den[h % 4, at, :] = sm
            top[h % 4, at, :] = score
        else:
            old = top[h % 4, at, :]
            new = jnp.maximum(old, score)
            keep = jnp.exp(old - new)
            take = jnp.exp(score - new)
            num[h % 4, at, :] = num[h % 4, at, :] * keep + got * take
            den[h % 4, at, :] = den[h % 4, at, :] * keep + sm * take
            top[h % 4, at, :] = new

    lane = lax.broadcasted_iota(jnp.int32, (LANE, LANE), 1)

    def send_o(a):
        return pltpu.make_async_remote_copy(o_own.at[a], o_oth.at[a], osend.at[a], orecv.at[a], device_id={'tp': 1 - tp}, device_id_type=MESH)

    def finish(h):
        a = h // 2
        limit = LANE - DIM * (h % 2)
        for pos in range(8):
            at = pl.ds(pl.multiple_of(((ORDER[pos] + h) % 8) * LANE, LANE), LANE)
            got = num[h % 4, pos * LANE:(pos + 1) * LANE, :] / den[h % 4, pos * LANE:(pos + 1) * LANE, :]
            o_own[a, at, :] = jnp.where(lane < limit, got, o_own[a, at, :].astype(F32)).astype(BF16)

    def unit_of(u, h):
        branch, shift, first, rows = UNITS[u]
        return branch, h + shift, first, rows

    def push(flight, unit):
        slot = (flight[-1][1] + 1) % SLOTS if flight else 0
        done = None
        if len(flight) == 2:
            gain(*flight[0])
            done = flight[0][0]
        logits(unit, slot)
        if flight:
            soften(*flight[-1])
        flight = flight[-1:]
        return flight + [(unit, slot)], done

    def run(flight, units):
        for unit in units:
            flight, done = push(flight, unit)
            if done is not None and done[0] == 3:
                finish(done[1])
        return flight

    def each(h, *which):
        return [unit_of(u, h) for u in which]

    event1(0)
    event2(0)
    arrive(0, 1)
    flight = run([], each(0, 0, 1, 2, 3))
    event3(0)
    event1(1)
    event2(1)
    flight = run(flight, each(0, 5, 6))
    arrive(1, 1)
    flight = run(flight, each(1, 0, 1, 2, 3))
    event4(0)
    event3(1)
    event1(2)
    event2(2)
    flight = run(flight, each(1, 4, 5, 6))

    def entering(h):
        return [(unit_of(5, h - 1), flight[0][1]), (unit_of(6, h - 1), flight[1][1])]

    def body(h, carry):
        arrive(h, 1)
        event4(h - 1)
        event3(h)
        event1(h + 1)
        event2(h + 1)

        @pl.when((h >= 4) & (h % 2 == 0))
        def _():
            send_o((h - 4) // 2).start()

        arrive_all(h - 2, 3)
        left = run(entering(h), [unit_of(7, h)] + each(h, 0, 1, 2, 3, 4, 5, 6))
        assert [f[1] for f in left] == [f[1] for f in flight]
        return carry

    lax.fori_loop(2, HEADS - 1, body, 0)
    last = HEADS - 1
    arrive(last, 1)
    event4(last - 1)
    event3(last)
    arrive_all(last - 2, 3)
    flight = run(entering(last), [unit_of(7, last)] + each(last, 0, 1, 2, 3))
    event4(last)
    send_o(2).start()
    flight = run(flight, each(last, 4, 5, 6))
    arrive_all(last - 1, 3)
    flight = run(flight, [unit_of(7, HEADS), unit_of(4, HEADS)])
    arrive_all(last, 3)
    flight = run(flight, [unit_of(7, HEADS + 1)])
    gain(*flight[0])
    soften(*flight[1])
    gain(*flight[1])
    finish(last)
    send_o(3).start()

    mine = pl.ds(pl.multiple_of(tp * HALF, HALF), HALF)

    def swapped(ref, cols):
        parts = []
        for a in range(4):
            parts += [ref[a * LANE + DIM:a * LANE + LANE, cols], ref[a * LANE:a * LANE + DIM, cols]]
        return jnp.concatenate(parts, axis=0)

    def heads_of(ref, half):
        return jnp.concatenate([ref[a, half * HALF:(half + 1) * HALF, :] for a in range(4)], axis=1)

    w_mine = swapped(wo_v, mine)
    for half in range(2):
        part_o[half * HALF:(half + 1) * HALF, :] = nn_dot(heads_of(o_own, half), w_mine)
    send_w.wait()
    for a in range(4):
        send_o(a).wait()
    w_other = swapped(wo_x, slice(None))
    for half in range(2):
        at = slice(half * HALF, (half + 1) * HALF)
        out[at, :] = (part_o[at, :] + nn_dot(heads_of(o_oth, half), w_other)).astype(BF16)
    for level in range(4):
        sent(level)


def restore(outp, out):
    row_id = lax.broadcasted_iota(jnp.int32, (LANE, LANE), 0)
    col_id = lax.broadcasted_iota(jnp.int32, (LANE, LANE), 1)
    spread = jnp.where(row_id == 8 * (col_id % 16) + col_id // 16, 1.0, 0.0).astype(BF16)
    for c in range(8):
        part = jnp.concatenate([outp[r * LANE + c * 16:r * LANE + (c + 1) * 16, :] for r in range(8)], axis=0)
        out[c * LANE:(c + 1) * LANE, :] = nn_dot(spread, part).astype(BF16)


def solution(mesh):
    def device_fn(hidden, w_query, w_key, w_value, w_out, branch_bias):
        kv = pltpu.VMEM((HEADS, ROWS, LANE), BF16)
        permuted = pl.pallas_call(
            kernel,
            out_shape=jax.ShapeDtypeStruct((ROWS, HALF), BF16),
            in_specs=[pl.BlockSpec(memory_space=pl.ANY)] * 5 + [pl.BlockSpec(memory_space=pltpu.SMEM)],
            out_specs=pl.BlockSpec(memory_space=pltpu.VMEM),
            scratch_shapes=[
                pltpu.VMEM((ROWS, 1024), BF16),
                pltpu.VMEM((1024, HALF), BF16), pltpu.VMEM((1024, HALF), BF16), pltpu.VMEM((1024, HALF), BF16),
                pltpu.VMEM((HALF, 1024), BF16), pltpu.VMEM((HALF, HALF), BF16),
                pltpu.VMEM((ROWS, 1024), BF16),
                kv, kv, kv, kv, kv, kv,
                *[pltpu.VMEM((TILE, KEYS), F32)] * SLOTS, *[pltpu.VMEM((TILE, KEYS), BF16)] * SLOTS,
                *[pltpu.VMEM((TILE, LANE), F32)] * (2 * SLOTS),
                pltpu.VMEM((4, ROWS, LANE), F32), pltpu.VMEM((4, ROWS, LANE), F32), pltpu.VMEM((4, ROWS, LANE), F32),
                pltpu.VMEM((4, ROWS, LANE), BF16), pltpu.VMEM((4, ROWS, LANE), BF16),
                pltpu.VMEM((ROWS, HALF), F32),
                pltpu.SemaphoreType.DMA((5,)),
                pltpu.SemaphoreType.DMA((4,)), pltpu.SemaphoreType.DMA((HEADS, 6)),
                pltpu.SemaphoreType.DMA((5,)), pltpu.SemaphoreType.DMA((5,)),
            ],
            compiler_params=pltpu.CompilerParams(collective_id=0, has_side_effects=True, vmem_limit_bytes=62 * 1024 * 1024),
            name='dilated',
        )(hidden, w_query, w_key, w_value, w_out, branch_bias)
        return pl.pallas_call(
            restore,
            out_shape=jax.ShapeDtypeStruct((ROWS, HALF), BF16),
            in_specs=[pl.BlockSpec(memory_space=pltpu.VMEM)],
            out_specs=pl.BlockSpec(memory_space=pltpu.VMEM),
            name='restore',
        )(permuted)

    return jax.shard_map(device_fn, mesh=mesh, in_specs=(P(('dp', 'sp'), None), P(None, 'tp'), P(None, 'tp'), P(None, 'tp'), P('tp', None), P(None, None)), out_specs=P(('dp', 'sp'), 'tp'), check_vma=False)
```

```python
import functools

import jax
import jax.numpy as jnp
from jax import lax
from jax.experimental import pallas as pl
from jax.experimental.pallas import tpu as pltpu
from jax.sharding import PartitionSpec as P

MESH = pl.DeviceIdType.MESH
F32 = jnp.float32
BF16 = jnp.bfloat16
ORDER = (0, 4, 2, 6, 1, 5, 3, 7)
HEADS = 8
ROWS = 1024
TILE = 256
LANE = 128
SUB = 8
HALF = 512
DIM = 64
KEYS = 2048
SLOTS = 2

UNITS = (
    (0, 0, 0, 256),
    (0, 0, 256, 256),
    (0, 0, 512, 256),
    (0, 0, 768, 256),
    (2, -1, 0, 256),
    (1, 0, 0, 256),
    (1, 0, 256, 256),
    (3, -2, 0, 128),
)


def nt_dot(a, b):
    return lax.dot_general(a, b, (((1,), (1,)), ((), ())), preferred_element_type=F32)


def tn_dot(a, b):
    return lax.dot_general(a, b, (((0,), (0,)), ((), ())), preferred_element_type=F32)


def nn_dot(a, b):
    return jnp.dot(a, b, preferred_element_type=F32)


def kernel(hid, wq, wk, wv, wo, bias, out, hid_v, wq_v, wk_v, wv_v, wo_v, wo_x, xp, q_s, own, r1, r2, r3, r4, *more):
    S, PR, M, L, T = (more[n * SLOTS:(n + 1) * SLOTS] for n in range(5))
    num, den, top, o_t, o_own, o_oth, part_o, in_sem, ssem, rsem, osend, orecv = more[5 * SLOTS:]
    tp = lax.axis_index('tp')
    sp = lax.axis_index('sp')
    x = sp % 4
    y = (sp // 4) % 4
    peers = (sp + 1 - 2 * (x % 2), sp + 3 - 2 * x, sp + 4 * (1 - 2 * (y % 2)), sp + 4 * (3 - 2 * y))

    loads = [pltpu.make_async_copy(a, b, in_sem.at[n]) for n, (a, b) in enumerate(((hid, hid_v), (wk, wk_v), (wv, wv_v), (wq, wq_v), (wo, wo_v)))]
    for load in loads:
        load.start()

    barrier = pltpu.get_barrier_semaphore()
    for peer in peers:
        pl.semaphore_signal(barrier, inc=1, device_id={'sp': peer}, device_id_type=MESH)
    pl.semaphore_signal(barrier, inc=1, device_id={'tp': 1 - tp}, device_id_type=MESH)

    def refs(n, h):
        if n == 0:
            return own.at[h, pl.ds(0, HALF)], r1.at[h, pl.ds(0, HALF)], 0
        if n == 1:
            return own.at[h, pl.ds(HALF, HALF)], r1.at[h, pl.ds(HALF, HALF)], 0
        if n == 2:
            return own.at[h, pl.ds(0, HALF)], r2.at[h, pl.ds(0, HALF)], 1
        if n == 3:
            return r1.at[h, pl.ds(0, HALF)], r2.at[h, pl.ds(HALF, HALF)], 1
        if n < 8:
            src = (own.at[h, pl.ds(0, TILE)], r1.at[h, pl.ds(0, TILE)], r2.at[h, pl.ds(0, TILE)], r2.at[h, pl.ds(HALF, TILE)])[n - 4]
            return src, r3.at[h, pl.ds((n - 4) * TILE, TILE)], 2
        if n < 12:
            src = (own.at[h, pl.ds(0, LANE)], r1.at[h, pl.ds(0, LANE)], r2.at[h, pl.ds(0, LANE)], r2.at[h, pl.ds(HALF, LANE)])[n - 8]
        else:
            src = r3.at[h, pl.ds((n - 12) * TILE, LANE)]
        return src, r4.at[h, pl.ds((n - 8) * LANE, LANE)], 3

    def copy(n, h):
        src, dst, level = refs(n, h)
        sem = n if n < 4 else level + 2
        return pltpu.make_async_remote_copy(src, dst, ssem.at[level], rsem.at[h, sem], device_id={'sp': peers[level]}, device_id_type=MESH)

    def start(h, *chunks):
        for n in chunks:
            copy(n, h).start()

    def arrive(h, n):
        copy(n, h).wait_recv()

    def arrive_all(h, level):
        dst = (r3, r4)[level - 2].at[h]
        pltpu.make_async_remote_copy(dst, dst, ssem.at[level], rsem.at[h, level + 2], device_id={'sp': peers[level]}, device_id_type=MESH).wait_recv()

    def sent(level):
        pltpu.make_async_remote_copy(own, own, ssem.at[level], rsem.at[0, 0], device_id={'sp': peers[level]}, device_id_type=MESH).wait_send()

    def event1(h):
        arrive(h, 0)
        start(h, 3, 5, 9)
        if isinstance(h, int):
            if h + 2 < HEADS:
                start(h + 2, 2, 4, 8)
        else:
            @pl.when(h + 2 < HEADS)
            def _():
                start(h + 2, 2, 4, 8)

    def event2(h):
        arrive(h, 2)
        start(h, 6, 10)

    def event3(h):
        arrive(h, 3)
        start(h, 7, 11)

    def event4(h):
        arrive_all(h, 2)
        start(h, 12, 13, 14, 15)

    row_id = lax.broadcasted_iota(jnp.int32, (LANE, LANE), 0)
    col_id = lax.broadcasted_iota(jnp.int32, (LANE, LANE), 1)
    gather = jnp.where(col_id == 8 * (row_id % 16) + row_id // 16, 1.0, 0.0).astype(BF16)

    loads[0].wait()
    for c in range(8):
        part = nn_dot(gather, hid_v[c * LANE:(c + 1) * LANE, :]).astype(BF16)
        for r in range(8):
            xp[r * LANE + c * 16:r * LANE + (c + 1) * 16, :] = part[r * 16:(r + 1) * 16, :]

    low = lax.broadcasted_iota(jnp.int32, (HALF, LANE), 1) < DIM

    def place(dst, h, half, value):
        for j in range(4):
            pos = ORDER.index((half * 4 + j - h) % 8)
            dst[h, pos * LANE:(pos + 1) * LANE, :] = value[j * LANE:(j + 1) * LANE, :]

    def project_kv(cols):
        for half in range(2):
            rows = xp[half * HALF:(half + 1) * HALF, :]
            key = nn_dot(rows, wk_v[:, cols * TILE:(cols + 1) * TILE])
            val = nn_dot(rows, wv_v[:, cols * TILE:(cols + 1) * TILE])
            for a in range(2):
                h = 4 * cols + 2 * a
                kp = key[:, a * LANE:(a + 1) * LANE]
                vp = pltpu.roll(val[:, a * LANE:(a + 1) * LANE], DIM, 1)
                place(own, h, half, jnp.where(low, kp, vp).astype(BF16))
                place(own, h + 1, half, jnp.where(low, vp, kp).astype(BF16))

    def project_q(cols):
        for half in range(2):
            qry = nn_dot(xp[half * HALF:(half + 1) * HALF, :], wq_v[:, cols * TILE:(cols + 1) * TILE]) * 0.125
            for a in range(2):
                h = 4 * cols + 2 * a
                qp = qry[:, a * LANE:(a + 1) * LANE]
                place(q_s, h, half, jnp.where(low, qp, 0.0).astype(BF16))
                place(q_s, h + 1, half, jnp.where(low, 0.0, qp).astype(BF16))

    loads[1].wait()
    loads[2].wait()
    project_kv(0)
    pl.semaphore_wait(barrier, 5)
    for h in range(2):
        start(h, 0, 1, 2, 4, 8)
    for h in range(2, 4):
        start(h, 0, 1)
    project_kv(1)
    for h in range(4, HEADS):
        start(h, 0, 1)
    loads[4].wait()
    send_w = pltpu.make_async_remote_copy(
        wo_v.at[:, pl.ds(pl.multiple_of((1 - tp) * HALF, HALF), HALF)], wo_x, osend.at[4], orecv.at[4],
        device_id={'tp': 1 - tp}, device_id_type=MESH)
    send_w.start()
    loads[3].wait()
    project_q(0)
    project_q(1)
    o_t[...] = jnp.zeros_like(o_t)

    def keys(branch, h):
        if branch == 0:
            parts = [own[h], r1[h]]
        elif branch == 1:
            parts = [own[h, 0:HALF, :], r1[h, 0:HALF, :], r2[h]]
        elif branch == 2:
            parts = [own[h, 0:TILE, :], r1[h, 0:TILE, :], r2[h, 0:TILE, :], r2[h, HALF:768, :], r3[h]]
        else:
            parts = [own[h, 0:LANE, :], r1[h, 0:LANE, :], r2[h, 0:LANE, :], r2[h, HALF:640, :]]
            parts += [r3[h, c * TILE:c * TILE + LANE, :] for c in range(4)] + [r4[h]]
        return jnp.concatenate(parts, axis=0)

    def logits(unit, slot):
        branch, h, first, rows = unit
        s = nt_dot(keys(branch, h), q_s[h, first:first + rows, :])
        S[slot][:, 0:rows] = s
        M[slot][:, 0:rows] = jnp.broadcast_to(jnp.max(s, axis=0, keepdims=True), (SUB, rows))

    def soften(unit, slot):
        rows = unit[3]
        m = M[slot][0:1, 0:rows]
        total = jnp.zeros((1, rows), F32)
        for c in range(KEYS // HALF):
            at = slice(c * HALF, (c + 1) * HALF)
            e = jnp.exp(S[slot][at, 0:rows] - m)
            PR[slot][at, 0:rows] = e.astype(BF16)
            total = total + jnp.sum(e, axis=0, keepdims=True)
        T[slot][:, 0:rows] = jnp.broadcast_to(m, (SUB, rows))
        L[slot][:, 0:rows] = jnp.broadcast_to(total, (SUB, rows))

    def gain(unit, slot):
        branch, h, first, rows = unit
        got = tn_dot(keys(branch, h), PR[slot][:, 0:rows])
        total = L[slot][:, 0:rows]
        at = slice(first, first + rows)
        score = T[slot][:, 0:rows] + bias[branch, tp * HEADS + h]
        if branch == 0:
            num[h % 4, :, at] = got
            den[h % 4, :, at] = total
            top[h % 4, :, at] = score
        else:
            old = top[h % 4, :, at]
            new = jnp.maximum(old, score)
            keep = jnp.exp(old - new)
            take = jnp.exp(score - new)
            num[h % 4, :, at] = num[h % 4, :, at] * keep[0:1, :] + got * take[0:1, :]
            den[h % 4, :, at] = den[h % 4, :, at] * keep + total * take
            top[h % 4, :, at] = new

    def send_o(a):
        return pltpu.make_async_remote_copy(o_own.at[a], o_oth.at[a], osend.at[a], orecv.at[a], device_id={'tp': 1 - tp}, device_id_type=MESH)

    def finish(h):
        a, odd = h // 2, h % 2
        have = pl.ds(pl.multiple_of((1 - odd) * DIM, DIM), DIM)
        want = pl.ds(pl.multiple_of(odd * DIM, DIM), DIM)
        for pos in range(8):
            at = slice(pos * LANE, (pos + 1) * LANE)
            to = pl.ds(pl.multiple_of(((ORDER[pos] + h) % 8) * LANE, LANE), LANE)
            o_t[a, want, to] = num[h % 4, have, at] / den[h % 4, 0:1, at]
        for r in range(8):
            at = slice(r * LANE, (r + 1) * LANE)
            o_own[a, at, :] = o_t[a, :, at].T.astype(BF16)

    def unit_of(u, h):
        branch, shift, first, rows = UNITS[u]
        return branch, h + shift, first, rows

    def push(flight, unit):
        slot = (flight[-1][1] + 1) % SLOTS if flight else 0
        pl.delay(1)
        logits(unit, slot)
        if flight:
            soften(*flight[-1])
            gain(*flight[-1])
        return [(unit, slot)], flight[-1][0] if flight else None

    def run(flight, units):
        for unit in units:
            flight, done = push(flight, unit)
            if done is not None and done[0] == 3:
                finish(done[1])
        return flight

    def each(h, *which):
        return [unit_of(u, h) for u in which]

    event1(0)
    event2(0)
    arrive(0, 1)
    flight = run([], each(0, 0, 1, 2, 3))
    event3(0)
    event1(1)
    event2(1)
    flight = run(flight, each(0, 5, 6))
    arrive(1, 1)
    flight = run(flight, each(1, 0, 1, 2, 3))
    event4(0)
    event3(1)
    event1(2)
    event2(2)
    flight = run(flight, each(1, 4, 5, 6))

    def entering(h):
        return [(unit_of(6, h - 1), flight[0][1])]

    def body(h, carry):
        arrive(h, 1)
        event4(h - 1)
        event3(h)
        event1(h + 1)
        event2(h + 1)

        @pl.when((h >= 4) & (h % 2 == 0))
        def _():
            send_o((h - 4) // 2).start()

        arrive_all(h - 2, 3)
        left = run(entering(h), [unit_of(7, h)] + each(h, 0, 1, 2, 3, 4, 5, 6))
        assert [f[1] for f in left] == [f[1] for f in flight]
        return carry

    lax.fori_loop(2, HEADS - 1, body, 0)
    last = HEADS - 1
    arrive(last, 1)
    event4(last - 1)
    event3(last)
    arrive_all(last - 2, 3)
    flight = run(entering(last), [unit_of(7, last)] + each(last, 0, 1, 2, 3))
    event4(last)
    send_o(2).start()
    flight = run(flight, each(last, 4, 5, 6))
    arrive_all(last - 1, 3)
    flight = run(flight, [unit_of(7, HEADS), unit_of(4, HEADS)])
    arrive_all(last, 3)
    flight = run(flight, [unit_of(7, HEADS + 1)])
    soften(*flight[0])
    gain(*flight[0])
    finish(last)
    send_o(3).start()

    mine = pl.ds(pl.multiple_of(tp * HALF, HALF), HALF)

    def heads_of(ref, half):
        return jnp.concatenate([ref[a, half * HALF:(half + 1) * HALF, :] for a in range(4)], axis=1)

    w_mine = wo_v[:, mine]
    for half in range(2):
        part_o[half * HALF:(half + 1) * HALF, :] = nn_dot(heads_of(o_own, half), w_mine)
    send_w.wait()
    for a in range(4):
        send_o(a).wait()
    w_other = wo_x[...]
    for half in range(2):
        at = slice(half * HALF, (half + 1) * HALF)
        out[at, :] = (part_o[at, :] + nn_dot(heads_of(o_oth, half), w_other)).astype(BF16)
    for level in range(4):
        sent(level)


def restore(outp, out):
    row_id = lax.broadcasted_iota(jnp.int32, (LANE, LANE), 0)
    col_id = lax.broadcasted_iota(jnp.int32, (LANE, LANE), 1)
    spread = jnp.where(row_id == 8 * (col_id % 16) + col_id // 16, 1.0, 0.0).astype(BF16)
    for c in range(8):
        part = jnp.concatenate([outp[r * LANE + c * 16:r * LANE + (c + 1) * 16, :] for r in range(8)], axis=0)
        out[c * LANE:(c + 1) * LANE, :] = nn_dot(spread, part).astype(BF16)


def solution(mesh):
    def device_fn(hidden, w_query, w_key, w_value, w_out, branch_bias):
        kv = pltpu.VMEM((HEADS, ROWS, LANE), BF16)
        permuted = pl.pallas_call(
            kernel,
            out_shape=jax.ShapeDtypeStruct((ROWS, HALF), BF16),
            in_specs=[pl.BlockSpec(memory_space=pl.ANY)] * 5 + [pl.BlockSpec(memory_space=pltpu.SMEM)],
            out_specs=pl.BlockSpec(memory_space=pltpu.VMEM),
            scratch_shapes=[
                pltpu.VMEM((ROWS, 1024), BF16),
                pltpu.VMEM((1024, HALF), BF16), pltpu.VMEM((1024, HALF), BF16), pltpu.VMEM((1024, HALF), BF16),
                pltpu.VMEM((HALF, 1024), BF16), pltpu.VMEM((HALF, HALF), BF16),
                pltpu.VMEM((ROWS, 1024), BF16),
                kv, kv, kv, kv, kv, kv,
                *[pltpu.VMEM((KEYS, TILE), F32)] * SLOTS, *[pltpu.VMEM((KEYS, TILE), BF16)] * SLOTS,
                *[pltpu.VMEM((SUB, TILE), F32)] * (3 * SLOTS),
                pltpu.VMEM((4, LANE, ROWS), F32), pltpu.VMEM((4, SUB, ROWS), F32), pltpu.VMEM((4, SUB, ROWS), F32), pltpu.VMEM((4, LANE, ROWS), F32),
                pltpu.VMEM((4, ROWS, LANE), BF16), pltpu.VMEM((4, ROWS, LANE), BF16),
                pltpu.VMEM((ROWS, HALF), F32),
                pltpu.SemaphoreType.DMA((5,)),
                pltpu.SemaphoreType.DMA((4,)), pltpu.SemaphoreType.DMA((HEADS, 6)),
                pltpu.SemaphoreType.DMA((5,)), pltpu.SemaphoreType.DMA((5,)),
            ],
            compiler_params=pltpu.CompilerParams(collective_id=0, has_side_effects=True, vmem_limit_bytes=62 * 1024 * 1024),
            name='dilated',
        )(hidden, w_query, w_key, w_value, w_out, branch_bias)
        return pl.pallas_call(
            restore,
            out_shape=jax.ShapeDtypeStruct((ROWS, HALF), BF16),
            in_specs=[pl.BlockSpec(memory_space=pltpu.VMEM)],
            out_specs=pl.BlockSpec(memory_space=pltpu.VMEM),
            name='restore',
        )(permuted)

    return jax.shard_map(device_fn, mesh=mesh, in_specs=(P(('dp', 'sp'), None), P(None, 'tp'), P(None, 'tp'), P(None, 'tp'), P('tp', None), P(None, None)), out_specs=P(('dp', 'sp'), 'tp'), check_vma=False)
```

```python
import functools

import jax
import jax.numpy as jnp
from jax import lax
from jax.experimental import pallas as pl
from jax.experimental.pallas import tpu as pltpu
from jax.sharding import PartitionSpec as P

MESH = pl.DeviceIdType.MESH
F32 = jnp.float32
BF16 = jnp.bfloat16
ORDER = (0, 4, 2, 6, 1, 5, 3, 7)
HEADS = 8
ROWS = 1024
TILE = 256
LANE = 128
SUB = 8
HALF = 512
DIM = 64
KEYS = 2048
SLOTS = 2

UNITS = (
    (0, 0, 0, TILE),
    (0, 0, TILE, TILE),
    (0, 0, 2 * TILE, TILE),
    (0, 0, 3 * TILE, TILE),
    (2, -1, 0, TILE),
    (1, 0, 0, TILE),
    (1, 0, TILE, TILE),
    (3, -1, 0, LANE),
)


def nt_dot(a, b):
    return lax.dot_general(a, b, (((1,), (1,)), ((), ())), preferred_element_type=F32)


def tn_dot(a, b):
    return lax.dot_general(a, b, (((0,), (0,)), ((), ())), preferred_element_type=F32)


def nn_dot(a, b):
    return jnp.dot(a, b, preferred_element_type=F32)


def kernel(hid, wq, wk, wv, wo, bias, out, hid_v, wq_v, wk_v, wv_v, wo_v, wo_x, xp, q_s, own, r1, r2, r3, r4, *more):
    S, PR, M, L, T = (more[n * SLOTS:(n + 1) * SLOTS] for n in range(5))
    num, den, top, o_t, o_own, o_oth, part_o, in_sem, ssem, rsem, osend, orecv = more[5 * SLOTS:]
    tp = lax.axis_index('tp')
    sp = lax.axis_index('sp')
    x = sp % 4
    y = (sp // 4) % 4
    peers = (sp + 1 - 2 * (x % 2), sp + 3 - 2 * x, sp + 4 * (1 - 2 * (y % 2)), sp + 4 * (3 - 2 * y))

    loads = [pltpu.make_async_copy(a, b, in_sem.at[n]) for n, (a, b) in enumerate(((hid, hid_v), (wk, wk_v), (wv, wv_v), (wq, wq_v), (wo, wo_v)))]
    for load in loads:
        load.start()

    barrier = pltpu.get_barrier_semaphore()
    for peer in peers:
        pl.semaphore_signal(barrier, inc=1, device_id={'sp': peer}, device_id_type=MESH)
    pl.semaphore_signal(barrier, inc=1, device_id={'tp': 1 - tp}, device_id_type=MESH)

    def refs(n, h):
        if n == 0:
            return own.at[h, pl.ds(0, HALF)], r1.at[h, pl.ds(0, HALF)], 0
        if n == 1:
            return own.at[h, pl.ds(HALF, HALF)], r1.at[h, pl.ds(HALF, HALF)], 0
        if n == 2:
            return own.at[h, pl.ds(0, HALF)], r2.at[h, pl.ds(0, HALF)], 1
        if n == 3:
            return r1.at[h, pl.ds(0, HALF)], r2.at[h, pl.ds(HALF, HALF)], 1
        if n < 8:
            src = (own.at[h, pl.ds(0, TILE)], r1.at[h, pl.ds(0, TILE)], r2.at[h, pl.ds(0, TILE)], r2.at[h, pl.ds(HALF, TILE)])[n - 4]
            return src, r3.at[h, pl.ds((n - 4) * TILE, TILE)], 2
        if n < 12:
            src = (own.at[h, pl.ds(0, LANE)], r1.at[h, pl.ds(0, LANE)], r2.at[h, pl.ds(0, LANE)], r2.at[h, pl.ds(HALF, LANE)])[n - 8]
        else:
            src = r3.at[h, pl.ds((n - 12) * TILE, LANE)]
        return src, r4.at[h, pl.ds((n - 8) * LANE, LANE)], 3

    def copy(n, h):
        src, dst, level = refs(n, h)
        sem = min(n, 8)
        return pltpu.make_async_remote_copy(src, dst, ssem.at[level], rsem.at[h, sem], device_id={'sp': peers[level]}, device_id_type=MESH)

    def start(h, *chunks):
        for n in chunks:
            copy(n, h).start()

    def arrive(h, n):
        copy(n, h).wait_recv()

    def arrive_all(h):
        pltpu.make_async_remote_copy(r4.at[h], r4.at[h], ssem.at[3], rsem.at[h, 8], device_id={'sp': peers[3]}, device_id_type=MESH).wait_recv()

    def sent(level):
        pltpu.make_async_remote_copy(own, own, ssem.at[level], rsem.at[0, 0], device_id={'sp': peers[level]}, device_id_type=MESH).wait_send()

    def event1(h):
        arrive(h, 0)
        start(h, 3, 5, 9)
        if isinstance(h, int):
            if h + 2 < HEADS:
                start(h + 2, 2, 4, 8)
        else:
            @pl.when(h + 2 < HEADS)
            def _():
                start(h + 2, 2, 4, 8)

    def event2(h):
        arrive(h, 2)
        start(h, 6, 10)

    def event3(h):
        arrive(h, 3)
        start(h, 7, 11)

    def event4(h, *parts):
        for c in parts:
            arrive(h, 4 + c)
            start(h, 12 + c)

    row_id = lax.broadcasted_iota(jnp.int32, (LANE, LANE), 0)
    col_id = lax.broadcasted_iota(jnp.int32, (LANE, LANE), 1)
    gather = jnp.where(col_id == 8 * (row_id % 16) + row_id // 16, 1.0, 0.0).astype(BF16)

    loads[0].wait()
    for c in range(8):
        part = nn_dot(gather, hid_v[c * LANE:(c + 1) * LANE, :]).astype(BF16)
        for r in range(8):
            xp[r * LANE + c * 16:r * LANE + (c + 1) * 16, :] = part[r * 16:(r + 1) * 16, :]

    low = lax.broadcasted_iota(jnp.int32, (HALF, LANE), 1) < DIM

    def place(dst, h, half, value):
        for j in range(4):
            pos = ORDER.index((half * 4 + j - h) % 8)
            dst[h, pos * LANE:(pos + 1) * LANE, :] = value[j * LANE:(j + 1) * LANE, :]

    def project_kv(cols):
        for half in range(2):
            rows = xp[half * HALF:(half + 1) * HALF, :]
            key = nn_dot(rows, wk_v[:, cols * TILE:(cols + 1) * TILE])
            val = nn_dot(rows, wv_v[:, cols * TILE:(cols + 1) * TILE])
            for a in range(2):
                h = 4 * cols + 2 * a
                kp = key[:, a * LANE:(a + 1) * LANE]
                vp = pltpu.roll(val[:, a * LANE:(a + 1) * LANE], DIM, 1)
                place(own, h, half, jnp.where(low, kp, vp).astype(BF16))
                place(own, h + 1, half, jnp.where(low, vp, kp).astype(BF16))

    def project_q(cols):
        for half in range(2):
            qry = nn_dot(xp[half * HALF:(half + 1) * HALF, :], wq_v[:, cols * TILE:(cols + 1) * TILE]) * 0.125
            for a in range(2):
                h = 4 * cols + 2 * a
                qp = qry[:, a * LANE:(a + 1) * LANE]
                place(q_s, h, half, jnp.where(low, qp, 0.0).astype(BF16))
                place(q_s, h + 1, half, jnp.where(low, 0.0, qp).astype(BF16))

    loads[1].wait()
    loads[2].wait()
    project_kv(0)
    pl.semaphore_wait(barrier, 5)
    for h in range(2):
        start(h, 0, 1, 2, 4, 8)
    for h in range(2, 4):
        start(h, 0, 1)
    project_kv(1)
    for h in range(4, HEADS):
        start(h, 0, 1)
    loads[4].wait()
    send_w = pltpu.make_async_remote_copy(
        wo_v.at[:, pl.ds(pl.multiple_of((1 - tp) * HALF, HALF), HALF)], wo_x, osend.at[4], orecv.at[4],
        device_id={'tp': 1 - tp}, device_id_type=MESH)
    send_w.start()
    loads[3].wait()
    project_q(0)
    project_q(1)
    o_t[...] = jnp.zeros_like(o_t)

    def keys(branch, h):
        if branch == 0:
            parts = [own[h], r1[h]]
        elif branch == 1:
            parts = [own[h, 0:HALF, :], r1[h, 0:HALF, :], r2[h]]
        elif branch == 2:
            parts = [own[h, 0:TILE, :], r1[h, 0:TILE, :], r2[h, 0:TILE, :], r2[h, HALF:768, :], r3[h]]
        else:
            parts = [own[h, 0:LANE, :], r1[h, 0:LANE, :], r2[h, 0:LANE, :], r2[h, HALF:640, :]]
            parts += [r3[h, c * TILE:c * TILE + LANE, :] for c in range(4)] + [r4[h]]
        return jnp.concatenate(parts, axis=0)

    def logits(unit, slot):
        branch, h, first, rows = unit
        s = nt_dot(keys(branch, h), q_s[h, first:first + rows, :])
        S[slot][:, 0:rows] = s
        M[slot][:, 0:rows] = jnp.broadcast_to(jnp.max(s, axis=0, keepdims=True), (SUB, rows))

    def soften(unit, slot):
        rows = unit[3]
        m = M[slot][0:1, 0:rows]
        total = jnp.zeros((1, rows), F32)
        for c in range(KEYS // HALF):
            at = slice(c * HALF, (c + 1) * HALF)
            e = jnp.exp(S[slot][at, 0:rows] - m)
            PR[slot][at, 0:rows] = e.astype(BF16)
            total = total + jnp.sum(e, axis=0, keepdims=True)
        T[slot][:, 0:rows] = jnp.broadcast_to(m, (SUB, rows))
        L[slot][:, 0:rows] = jnp.broadcast_to(total, (SUB, rows))

    def gain(unit, slot):
        branch, h, first, rows = unit
        got = tn_dot(keys(branch, h), PR[slot][:, 0:rows])
        total = L[slot][:, 0:rows]
        at = slice(first, first + rows)
        score = T[slot][:, 0:rows] + bias[branch, tp * HEADS + h]
        if branch == 0:
            num[h % 4, :, at] = got
            den[h % 4, :, at] = total
            top[h % 4, :, at] = score
        else:
            old = top[h % 4, :, at]
            new = jnp.maximum(old, score)
            keep = jnp.exp(old - new)
            take = jnp.exp(score - new)
            num[h % 4, :, at] = num[h % 4, :, at] * keep[0:1, :] + got * take[0:1, :]
            den[h % 4, :, at] = den[h % 4, :, at] * keep + total * take
            top[h % 4, :, at] = new

    def send_o(a):
        return pltpu.make_async_remote_copy(o_own.at[a], o_oth.at[a], osend.at[a], orecv.at[a], device_id={'tp': 1 - tp}, device_id_type=MESH)

    def finish(h):
        a, odd = h // 2, h % 2
        have = pl.ds(pl.multiple_of((1 - odd) * DIM, DIM), DIM)
        want = pl.ds(pl.multiple_of(odd * DIM, DIM), DIM)
        for pos in range(8):
            at = slice(pos * LANE, (pos + 1) * LANE)
            to = pl.ds(pl.multiple_of(((ORDER[pos] + h) % 8) * LANE, LANE), LANE)
            o_t[a, want, to] = num[h % 4, have, at] / den[h % 4, 0:1, at]
        for r in range(8):
            at = slice(r * LANE, (r + 1) * LANE)
            o_own[a, at, :] = o_t[a, :, at].T.astype(BF16)

    def unit_of(u, h):
        branch, shift, first, rows = UNITS[u]
        return branch, h + shift, first, rows

    def push(flight, unit):
        slot = (flight[-1][1] + 1) % SLOTS if flight else 0
        pl.delay(1)
        logits(unit, slot)
        if flight:
            soften(*flight[-1])
            gain(*flight[-1])
        return [(unit, slot)], flight[-1][0] if flight else None

    def run(flight, h, *which):
        for u in which:
            flight, done = push(flight, unit_of(u, h))
            if done is not None and done[0] == 3:
                finish(done[1])
        return flight

    event1(0)
    event2(0)
    arrive(0, 1)
    flight = run([], 0, 0)
    event2(1)
    flight = run(flight, 0, 1, 2, 3)
    event3(0)
    event1(1)
    event4(0, 0, 1, 2)
    flight = run(flight, 0, 5, 6)

    def guard(condition, action):
        if not isinstance(condition, bool):
            pl.when(condition)(action)
        elif condition:
            action()

    def pass_of(h, flight):
        arrive(h, 1)
        flight = run(flight, h, 0)
        guard(h + 1 < HEADS, lambda: event2(h + 1))
        guard((h >= 3) & (h % 2 == 1), lambda: send_o((h - 3) // 2).start())
        flight = run(flight, h, 1)
        event4(h - 1, 3)
        flight = run(flight, h, 2, 3, 4)
        event3(h)
        guard(h + 1 < HEADS, lambda: event1(h + 1))
        event4(h, 0, 1, 2)
        flight = run(flight, h, 5, 6)
        arrive_all(h - 1)
        return run(flight, h, 7)

    flight = pass_of(1, flight)

    def body(h, carry):
        left = pass_of(h, [(unit_of(7, h - 1), flight[0][1])])
        assert left[0][1] == flight[0][1]
        return carry

    lax.fori_loop(2, HEADS, body, 0)
    flight = [(unit_of(7, HEADS - 1), flight[0][1])]
    event4(HEADS - 1, 3)
    flight = run(flight, HEADS, 4)
    arrive_all(HEADS - 1)
    flight = run(flight, HEADS, 7)
    soften(*flight[0])
    gain(*flight[0])
    finish(HEADS - 1)
    send_o(3).start()

    mine = pl.ds(pl.multiple_of(tp * HALF, HALF), HALF)

    def heads_of(ref, half):
        return jnp.concatenate([ref[a, half * HALF:(half + 1) * HALF, :] for a in range(4)], axis=1)

    w_mine = wo_v[:, mine]
    for half in range(2):
        part_o[half * HALF:(half + 1) * HALF, :] = nn_dot(heads_of(o_own, half), w_mine)
    send_w.wait()
    for a in range(4):
        send_o(a).wait()
    w_other = wo_x[...]
    for half in range(2):
        at = slice(half * HALF, (half + 1) * HALF)
        out[at, :] = (part_o[at, :] + nn_dot(heads_of(o_oth, half), w_other)).astype(BF16)
    for level in range(4):
        sent(level)


def restore(outp, out):
    row_id = lax.broadcasted_iota(jnp.int32, (LANE, LANE), 0)
    col_id = lax.broadcasted_iota(jnp.int32, (LANE, LANE), 1)
    spread = jnp.where(row_id == 8 * (col_id % 16) + col_id // 16, 1.0, 0.0).astype(BF16)
    for c in range(8):
        part = jnp.concatenate([outp[r * LANE + c * 16:r * LANE + (c + 1) * 16, :] for r in range(8)], axis=0)
        out[c * LANE:(c + 1) * LANE, :] = nn_dot(spread, part).astype(BF16)


def solution(mesh):
    def device_fn(hidden, w_query, w_key, w_value, w_out, branch_bias):
        kv = pltpu.VMEM((HEADS, ROWS, LANE), BF16)
        permuted = pl.pallas_call(
            kernel,
            out_shape=jax.ShapeDtypeStruct((ROWS, HALF), BF16),
            in_specs=[pl.BlockSpec(memory_space=pl.ANY)] * 5 + [pl.BlockSpec(memory_space=pltpu.SMEM)],
            out_specs=pl.BlockSpec(memory_space=pltpu.VMEM),
            scratch_shapes=[
                pltpu.VMEM((ROWS, 1024), BF16),
                pltpu.VMEM((1024, HALF), BF16), pltpu.VMEM((1024, HALF), BF16), pltpu.VMEM((1024, HALF), BF16),
                pltpu.VMEM((HALF, 1024), BF16), pltpu.VMEM((HALF, HALF), BF16),
                pltpu.VMEM((ROWS, 1024), BF16),
                kv, kv, kv, kv, kv, kv,
                *[pltpu.VMEM((KEYS, TILE), F32)] * SLOTS, *[pltpu.VMEM((KEYS, TILE), BF16)] * SLOTS,
                *[pltpu.VMEM((SUB, TILE), F32)] * (3 * SLOTS),
                pltpu.VMEM((4, LANE, ROWS), F32), pltpu.VMEM((4, SUB, ROWS), F32), pltpu.VMEM((4, SUB, ROWS), F32), pltpu.VMEM((4, LANE, ROWS), F32),
                pltpu.VMEM((4, ROWS, LANE), BF16), pltpu.VMEM((4, ROWS, LANE), BF16),
                pltpu.VMEM((ROWS, HALF), F32),
                pltpu.SemaphoreType.DMA((5,)),
                pltpu.SemaphoreType.DMA((4,)), pltpu.SemaphoreType.DMA((HEADS, 9)),
                pltpu.SemaphoreType.DMA((5,)), pltpu.SemaphoreType.DMA((5,)),
            ],
            compiler_params=pltpu.CompilerParams(collective_id=0, has_side_effects=True, vmem_limit_bytes=62 * 1024 * 1024),
            name='dilated',
        )(hidden, w_query, w_key, w_value, w_out, branch_bias)
        return pl.pallas_call(
            restore,
            out_shape=jax.ShapeDtypeStruct((ROWS, HALF), BF16),
            in_specs=[pl.BlockSpec(memory_space=pltpu.VMEM)],
            out_specs=pl.BlockSpec(memory_space=pltpu.VMEM),
            name='restore',
        )(permuted)

    return jax.shard_map(device_fn, mesh=mesh, in_specs=(P(('dp', 'sp'), None), P(None, 'tp'), P(None, 'tp'), P(None, 'tp'), P('tp', None), P(None, None)), out_specs=P(('dp', 'sp'), 'tp'), check_vma=False)
```

```python
import functools

import jax
import jax.numpy as jnp
from jax import lax
from jax.experimental import pallas as pl
from jax.experimental.pallas import tpu as pltpu
from jax.sharding import PartitionSpec as P

MESH = pl.DeviceIdType.MESH
F32 = jnp.float32
BF16 = jnp.bfloat16
ORDER = (0, 4, 2, 6, 1, 5, 3, 7)
HEADS = 8
ROWS = 1024
TILE = 256
LANE = 128
SUB = 8
HALF = 512
DIM = 64
KEYS = 2048
SLOTS = 3

UNITS = (
    (0, 0, 0, HALF),
    (0, 0, HALF, HALF),
    (2, -1, 0, TILE),
    (1, 0, 0, HALF),
    (3, -1, 0, LANE),
)
WIDTHS = (HALF, HALF, TILE)
SLOT_OF = (0, 1, 2, 0, 2)
SWAPPED = (1, 0, 2, 1, 2)


def nt_dot(a, b):
    return lax.dot_general(a, b, (((1,), (1,)), ((), ())), preferred_element_type=F32)


def tn_dot(a, b):
    return lax.dot_general(a, b, (((0,), (0,)), ((), ())), preferred_element_type=F32)


def nn_dot(a, b):
    return jnp.dot(a, b, preferred_element_type=F32)


def kernel(hid, wq, wk, wv, wo, bias, out, hid_v, wq_v, wk_v, wv_v, wo_v, wo_x, xp, q_s, own, r1, r2, r3, r4, *more):
    S, PR, M, L, T = (more[n * SLOTS:(n + 1) * SLOTS] for n in range(5))
    num, den, top, o_t, o_own, o_oth, part_o, in_sem, ssem, rsem, osend, orecv = more[5 * SLOTS:]
    tp = lax.axis_index('tp')
    sp = lax.axis_index('sp')
    x = sp % 4
    y = (sp // 4) % 4
    peers = (sp + 1 - 2 * (x % 2), sp + 3 - 2 * x, sp + 4 * (1 - 2 * (y % 2)), sp + 4 * (3 - 2 * y))

    loads = [pltpu.make_async_copy(a, b, in_sem.at[n]) for n, (a, b) in enumerate(((hid, hid_v), (wk, wk_v), (wv, wv_v), (wq, wq_v), (wo, wo_v)))]
    for load in loads:
        load.start()

    barrier = pltpu.get_barrier_semaphore()
    for peer in peers:
        pl.semaphore_signal(barrier, inc=1, device_id={'sp': peer}, device_id_type=MESH)
    pl.semaphore_signal(barrier, inc=1, device_id={'tp': 1 - tp}, device_id_type=MESH)

    def refs(n, h):
        low4, low2 = pl.ds(0, 4), pl.ds(0, 2)
        return (
            lambda: (own.at[h, low4], r1.at[h, low4], 0),
            lambda: (own.at[h, pl.ds(4, 4)], r1.at[h, pl.ds(4, 4)], 0),
            lambda: (own.at[h, low4], r2.at[h, :, 0], 1),
            lambda: (r1.at[h, low4], r2.at[h, :, 1], 1),
            lambda: (own.at[h, low2], r3.at[h, :, 0], 2),
            lambda: (r1.at[h, low2], r3.at[h, :, 1], 2),
            lambda: (r2.at[h, low2], r3.at[h, :, pl.ds(2, 2)], 2),
            lambda: (own.at[h, 0], r4.at[h, 0], 3),
            lambda: (r1.at[h, 0], r4.at[h, 1], 3),
            lambda: (r2.at[h, 0], r4.at[h, pl.ds(2, 2)], 3),
            lambda: (r3.at[h, 0, low2], r4.at[h, pl.ds(4, 2)], 3),
            lambda: (r3.at[h, 0, pl.ds(2, 2)], r4.at[h, pl.ds(6, 2)], 3),
        )[n]()

    def copy(n, h):
        src, dst, level = refs(n, h)
        sem = min(n, 7)
        return pltpu.make_async_remote_copy(src, dst, ssem.at[level], rsem.at[h, sem], device_id={'sp': peers[level]}, device_id_type=MESH)

    def start(h, *chunks):
        for n in chunks:
            copy(n, h).start()

    def arrive(h, n):
        copy(n, h).wait_recv()

    def arrive_all(h):
        pltpu.make_async_remote_copy(r4.at[h], r4.at[h], ssem.at[3], rsem.at[h, 7], device_id={'sp': peers[3]}, device_id_type=MESH).wait_recv()

    def sent(level):
        pltpu.make_async_remote_copy(own, own, ssem.at[level], rsem.at[0, 0], device_id={'sp': peers[level]}, device_id_type=MESH).wait_send()

    def event1(h):
        arrive(h, 0)
        start(h, 3, 5, 8)
        guard(h + 2 < HEADS, lambda: start(h + 2, 2, 4, 7))

    def event3(h):
        arrive(h, 2)
        arrive(h, 3)
        start(h, 6, 9)

    def event4(h):
        arrive(h, 4)
        arrive(h, 5)
        start(h, 10)

    def event5(h):
        arrive(h, 6)
        start(h, 11)

    def guard(condition, action):
        if not isinstance(condition, bool):
            pl.when(condition)(action)
        elif condition:
            action()

    row_id = lax.broadcasted_iota(jnp.int32, (LANE, LANE), 0)
    col_id = lax.broadcasted_iota(jnp.int32, (LANE, LANE), 1)
    gather = jnp.where(col_id == 8 * (row_id % 16) + row_id // 16, 1.0, 0.0).astype(BF16)

    loads[0].wait()
    for c in range(8):
        part = nn_dot(gather, hid_v[c * LANE:(c + 1) * LANE, :]).astype(BF16)
        for r in range(8):
            xp[r * LANE + c * 16:r * LANE + (c + 1) * 16, :] = part[r * 16:(r + 1) * 16, :]

    low = lax.broadcasted_iota(jnp.int32, (HALF, LANE), 1) < DIM

    def place(dst, h, half, value):
        for j in range(4):
            pos = ORDER.index((half * 4 + j - h) % 8)
            dst[h, pos] = value[j * LANE:(j + 1) * LANE, :]

    def project_kv(cols):
        for half in range(2):
            rows = xp[half * HALF:(half + 1) * HALF, :]
            key = nn_dot(rows, wk_v[:, cols * TILE:(cols + 1) * TILE])
            val = nn_dot(rows, wv_v[:, cols * TILE:(cols + 1) * TILE])
            for a in range(2):
                h = 4 * cols + 2 * a
                kp = key[:, a * LANE:(a + 1) * LANE]
                vp = pltpu.roll(val[:, a * LANE:(a + 1) * LANE], DIM, 1)
                place(own, h, half, jnp.where(low, kp, vp).astype(BF16))
                place(own, h + 1, half, jnp.where(low, vp, kp).astype(BF16))

    def project_q(cols):
        for half in range(2):
            qry = nn_dot(xp[half * HALF:(half + 1) * HALF, :], wq_v[:, cols * TILE:(cols + 1) * TILE]) * 0.125
            for a in range(2):
                h = 4 * cols + 2 * a
                qp = qry[:, a * LANE:(a + 1) * LANE]
                place(q_s, h, half, jnp.where(low, qp, 0.0).astype(BF16))
                place(q_s, h + 1, half, jnp.where(low, 0.0, qp).astype(BF16))

    loads[1].wait()
    loads[2].wait()
    project_kv(0)
    pl.semaphore_wait(barrier, 5)
    for h in range(2):
        start(h, 0, 1, 2, 4, 7)
    for h in range(2, 4):
        start(h, 0, 1)
    project_kv(1)
    for h in range(4, HEADS):
        start(h, 0, 1)
    loads[4].wait()
    send_w = pltpu.make_async_remote_copy(
        wo_v.at[:, pl.ds(pl.multiple_of((1 - tp) * HALF, HALF), HALF)], wo_x, osend.at[4], orecv.at[4],
        device_id={'tp': 1 - tp}, device_id_type=MESH)
    send_w.start()
    loads[3].wait()
    project_q(0)
    project_q(1)
    o_t[...] = jnp.zeros_like(o_t)

    def keys(branch, h):
        count = 8 >> branch
        parts = [own[h, 0:count], r1[h, 0:count]]
        for level, held in ((1, r2), (2, r3), (3, r4)):
            if branch > level:
                parts.append(held[h, 0:count])
            elif branch == level:
                parts.append(held[h])
        return jnp.concatenate([p.reshape(p.size // LANE, LANE) for p in parts], axis=0)

    def logits(unit, slot):
        branch, h, first, rows = unit
        s = nt_dot(keys(branch, h), q_s[h, first // LANE:(first + rows) // LANE].reshape(rows, LANE))
        S[slot][:, 0:rows] = s
        M[slot][:, 0:rows] = jnp.broadcast_to(jnp.max(s, axis=0, keepdims=True), (SUB, rows))

    def soften(unit, slot):
        rows = unit[3]
        m = M[slot][0:1, 0:rows]
        total = jnp.zeros((1, rows), F32)
        for c in range(KEYS // HALF):
            at = slice(c * HALF, (c + 1) * HALF)
            e = jnp.exp(S[slot][at, 0:rows] - m)
            PR[slot][at, 0:rows] = e.astype(BF16)
            total = total + jnp.sum(e, axis=0, keepdims=True)
        T[slot][:, 0:rows] = jnp.broadcast_to(m, (SUB, rows))
        L[slot][:, 0:rows] = jnp.broadcast_to(total, (SUB, rows))

    def gain(unit, slot):
        branch, h, first, rows = unit
        got = tn_dot(keys(branch, h), PR[slot][:, 0:rows])
        total = L[slot][:, 0:rows]
        at = slice(first, first + rows)
        score = T[slot][:, 0:rows] + bias[branch, tp * HEADS + h]
        if branch == 0:
            num[h % 4, :, at] = got
            den[h % 4, :, at] = total
            top[h % 4, :, at] = score
        else:
            old = top[h % 4, :, at]
            new = jnp.maximum(old, score)
            keep = jnp.exp(old - new)
            take = jnp.exp(score - new)
            num[h % 4, :, at] = num[h % 4, :, at] * keep[0:1, :] + got * take[0:1, :]
            den[h % 4, :, at] = den[h % 4, :, at] * keep + total * take
            top[h % 4, :, at] = new

    def send_o(a):
        return pltpu.make_async_remote_copy(o_own.at[a], o_oth.at[a], osend.at[a], orecv.at[a], device_id={'tp': 1 - tp}, device_id_type=MESH)

    def finish(h):
        a, odd = h // 2, h % 2
        have = pl.ds(pl.multiple_of((1 - odd) * DIM, DIM), DIM)
        want = pl.ds(pl.multiple_of(odd * DIM, DIM), DIM)
        for pos in range(8):
            at = slice(pos * LANE, (pos + 1) * LANE)
            to = pl.ds(pl.multiple_of(((ORDER[pos] + h) % 8) * LANE, LANE), LANE)
            o_t[a, want, to] = num[h % 4, have, at] / den[h % 4, 0:1, at]
        for r in range(8):
            at = slice(r * LANE, (r + 1) * LANE)
            o_own[a, at, :] = o_t[a, :, at].T.astype(BF16)

    def unit_of(u, h):
        branch, shift, first, rows = UNITS[u]
        return branch, h + shift, first, rows

    def push(flight, unit, slot):
        pl.delay(1)
        logits(unit, slot)
        if flight:
            soften(*flight[-1])
            gain(*flight[-1])
        return [(unit, slot)], flight[-1][0] if flight else None

    def run(flight, h, *which, slots=SLOT_OF):
        for u in which:
            flight, done = push(flight, unit_of(u, h), slots[u])
            if done is not None and done[0] == 3:
                finish(done[1])
        return flight

    event1(0)
    arrive(0, 1)
    flight = run([], 0, 0, 1, slots=SWAPPED)
    event3(0)
    event1(1)
    event4(0)
    flight = run(flight, 0, 3, slots=SWAPPED)

    def pass_of(h, flight):
        arrive(h, 1)
        flight = run(flight, h, 0)
        guard((h >= 3) & (h % 2 == 1), lambda: send_o((h - 3) // 2).start())
        event5(h - 1)
        flight = run(flight, h, 1, 2)
        event3(h)
        guard(h + 1 < HEADS, lambda: event1(h + 1))
        event4(h)
        flight = run(flight, h, 3)
        arrive_all(h - 1)
        return run(flight, h, 4)

    flight = pass_of(1, flight)

    def body(h, carry):
        left = pass_of(h, [(unit_of(4, h - 1), flight[0][1])])
        assert left[0][1] == flight[0][1]
        return carry

    lax.fori_loop(2, HEADS, body, 0)
    flight = [(unit_of(4, HEADS - 1), flight[0][1])]
    event5(HEADS - 1)
    flight = run(flight, HEADS, 2, slots=(0,) * 3)
    arrive_all(HEADS - 1)
    flight = run(flight, HEADS, 4)
    soften(*flight[0])
    gain(*flight[0])
    finish(HEADS - 1)
    send_o(3).start()

    mine = pl.ds(pl.multiple_of(tp * HALF, HALF), HALF)

    def heads_of(ref, half):
        return jnp.concatenate([ref[a, half * HALF:(half + 1) * HALF, :] for a in range(4)], axis=1)

    w_mine = wo_v[:, mine]
    for half in range(2):
        part_o[half * HALF:(half + 1) * HALF, :] = nn_dot(heads_of(o_own, half), w_mine)
    send_w.wait()
    for a in range(4):
        send_o(a).wait()
    w_other = wo_x[...]
    for half in range(2):
        at = slice(half * HALF, (half + 1) * HALF)
        out[at, :] = (part_o[at, :] + nn_dot(heads_of(o_oth, half), w_other)).astype(BF16)
    for level in range(4):
        sent(level)


def restore(outp, out):
    row_id = lax.broadcasted_iota(jnp.int32, (LANE, LANE), 0)
    col_id = lax.broadcasted_iota(jnp.int32, (LANE, LANE), 1)
    spread = jnp.where(row_id == 8 * (col_id % 16) + col_id // 16, 1.0, 0.0).astype(BF16)
    for c in range(8):
        part = jnp.concatenate([outp[r * LANE + c * 16:r * LANE + (c + 1) * 16, :] for r in range(8)], axis=0)
        out[c * LANE:(c + 1) * LANE, :] = nn_dot(spread, part).astype(BF16)


def solution(mesh):
    def device_fn(hidden, w_query, w_key, w_value, w_out, branch_bias):
        kv, kv2, kv3 = (pltpu.VMEM((HEADS, *lead, LANE, LANE), BF16) for lead in ((8,), (4, 2), (2, 4)))
        permuted = pl.pallas_call(
            kernel,
            out_shape=jax.ShapeDtypeStruct((ROWS, HALF), BF16),
            in_specs=[pl.BlockSpec(memory_space=pl.ANY)] * 5 + [pl.BlockSpec(memory_space=pltpu.SMEM)],
            out_specs=pl.BlockSpec(memory_space=pltpu.VMEM),
            scratch_shapes=[
                pltpu.VMEM((ROWS, 1024), BF16),
                pltpu.VMEM((1024, HALF), BF16), pltpu.VMEM((1024, HALF), BF16), pltpu.VMEM((1024, HALF), BF16),
                pltpu.VMEM((HALF, 1024), BF16), pltpu.VMEM((HALF, HALF), BF16),
                pltpu.VMEM((ROWS, 1024), BF16),
                kv, kv, kv, kv2, kv3, kv,
                *[pltpu.VMEM((KEYS, n), F32) for n in WIDTHS], *[pltpu.VMEM((KEYS, n), BF16) for n in WIDTHS],
                *[pltpu.VMEM((SUB, n), F32) for n in WIDTHS * 3],
                pltpu.VMEM((4, LANE, ROWS), F32), pltpu.VMEM((4, SUB, ROWS), F32), pltpu.VMEM((4, SUB, ROWS), F32), pltpu.VMEM((4, LANE, ROWS), F32),
                pltpu.VMEM((4, ROWS, LANE), BF16), pltpu.VMEM((4, ROWS, LANE), BF16),
                pltpu.VMEM((ROWS, HALF), F32),
                pltpu.SemaphoreType.DMA((5,)),
                pltpu.SemaphoreType.DMA((4,)), pltpu.SemaphoreType.DMA((HEADS, 8)),
                pltpu.SemaphoreType.DMA((5,)), pltpu.SemaphoreType.DMA((5,)),
            ],
            compiler_params=pltpu.CompilerParams(collective_id=0, has_side_effects=True, vmem_limit_bytes=62 * 1024 * 1024),
            name='dilated',
        )(hidden, w_query, w_key, w_value, w_out, branch_bias)
        return pl.pallas_call(
            restore,
            out_shape=jax.ShapeDtypeStruct((ROWS, HALF), BF16),
            in_specs=[pl.BlockSpec(memory_space=pltpu.VMEM)],
            out_specs=pl.BlockSpec(memory_space=pltpu.VMEM),
            name='restore',
        )(permuted)

    return jax.shard_map(device_fn, mesh=mesh, in_specs=(P(('dp', 'sp'), None), P(None, 'tp'), P(None, 'tp'), P(None, 'tp'), P('tp', None), P(None, None)), out_specs=P(('dp', 'sp'), 'tp'), check_vma=False)
```

```python
import functools

import jax
import jax.numpy as jnp
from jax import lax
from jax.experimental import pallas as pl
from jax.experimental.pallas import tpu as pltpu
from jax.sharding import PartitionSpec as P

MESH = pl.DeviceIdType.MESH
F32 = jnp.float32
BF16 = jnp.bfloat16
ORDER = (0, 4, 2, 6, 1, 5, 3, 7)
HEADS = 8
ROWS = 1024
TILE = 256
LANE = 128
SUB = 8
HALF = 512
DIM = 64
KEYS = 2048
SLOTS = 2

UNITS = (
    (0, 0, 0, TILE),
    (0, 0, TILE, TILE),
    (0, 0, 2 * TILE, TILE),
    (0, 0, 3 * TILE, TILE),
    (2, -1, 0, TILE),
    (1, 0, 0, TILE),
    (1, 0, TILE, TILE),
    (3, -1, 0, LANE),
)


def nt_dot(a, b):
    return lax.dot_general(a, b, (((1,), (1,)), ((), ())), preferred_element_type=F32)


def tn_dot(a, b):
    return lax.dot_general(a, b, (((0,), (0,)), ((), ())), preferred_element_type=F32)


def nn_dot(a, b):
    return jnp.dot(a, b, preferred_element_type=F32)


def kernel(hid, wq, wk, wv, wo, bias, out, hid_v, wq_v, wk_v, wv_v, wo_v, wo_x, xp, q_s, own, r1, r2, r3, r4, *more):
    S, PR, M, L, T = (more[n * SLOTS:(n + 1) * SLOTS] for n in range(5))
    num, den, top, o_t, o_own, o_oth, part_o, in_sem, ssem, rsem, osend, orecv = more[5 * SLOTS:]
    tp = lax.axis_index('tp')
    sp = lax.axis_index('sp')
    x = sp % 4
    y = (sp // 4) % 4
    peers = (sp + 1 - 2 * (x % 2), sp + 3 - 2 * x, sp + 4 * (1 - 2 * (y % 2)), sp + 4 * (3 - 2 * y))

    loads = [pltpu.make_async_copy(a, b, in_sem.at[n]) for n, (a, b) in enumerate(((hid, hid_v), (wk, wk_v), (wv, wv_v), (wq, wq_v), (wo, wo_v)))]
    for load in loads[:3]:
        load.start()

    barrier = pltpu.get_barrier_semaphore()
    for peer in peers:
        pl.semaphore_signal(barrier, inc=1, device_id={'sp': peer}, device_id_type=MESH)
    pl.semaphore_signal(barrier, inc=1, device_id={'tp': 1 - tp}, device_id_type=MESH)

    def refs(n, h):
        if n == 0:
            return own.at[h, pl.ds(0, HALF)], r1.at[h, pl.ds(0, HALF)], 0
        if n == 1:
            return own.at[h, pl.ds(HALF, HALF)], r1.at[h, pl.ds(HALF, HALF)], 0
        if n == 2:
            return own.at[h, pl.ds(0, HALF)], r2.at[h, pl.ds(0, HALF)], 1
        if n == 3:
            return r1.at[h, pl.ds(0, HALF)], r2.at[h, pl.ds(HALF, HALF)], 1
        if n < 8:
            src = (own.at[h, pl.ds(0, TILE)], r1.at[h, pl.ds(0, TILE)], r2.at[h, pl.ds(0, TILE)], r2.at[h, pl.ds(HALF, TILE)])[n - 4]
            return src, r3.at[h, pl.ds((n - 4) * TILE, TILE)], 2
        if n < 12:
            src = (own.at[h, pl.ds(0, LANE)], r1.at[h, pl.ds(0, LANE)], r2.at[h, pl.ds(0, LANE)], r2.at[h, pl.ds(HALF, LANE)])[n - 8]
        else:
            src = r3.at[h, pl.ds((n - 12) * TILE, LANE)]
        return src, r4.at[h, pl.ds((n - 8) * LANE, LANE)], 3

    def copy(n, h):
        src, dst, level = refs(n, h)
        sem = min(n, 8)
        return pltpu.make_async_remote_copy(src, dst, ssem.at[level], rsem.at[h, sem], device_id={'sp': peers[level]}, device_id_type=MESH)

    def start(h, *chunks):
        for n in chunks:
            copy(n, h).start()

    def arrive(h, n):
        copy(n, h).wait_recv()

    def arrive_all(h):
        pltpu.make_async_remote_copy(r4.at[h], r4.at[h], ssem.at[3], rsem.at[h, 8], device_id={'sp': peers[3]}, device_id_type=MESH).wait_recv()

    def sent(level):
        pltpu.make_async_remote_copy(own, own, ssem.at[level], rsem.at[0, 0], device_id={'sp': peers[level]}, device_id_type=MESH).wait_send()

    def event1(h):
        arrive(h, 0)
        start(h, 3, 5, 9)
        if isinstance(h, int):
            if h + 2 < HEADS:
                start(h + 2, 2, 4, 8)
        else:
            @pl.when(h + 2 < HEADS)
            def _():
                start(h + 2, 2, 4, 8)

    def event2(h):
        arrive(h, 2)
        start(h, 6, 10)

    def event3(h):
        arrive(h, 3)
        start(h, 7, 11)

    def event4(h, *parts):
        for c in parts:
            arrive(h, 4 + c)
            start(h, 12 + c)

    row_id = lax.broadcasted_iota(jnp.int32, (LANE, LANE), 0)
    col_id = lax.broadcasted_iota(jnp.int32, (LANE, LANE), 1)
    gather = jnp.where(col_id == 8 * (row_id % 16) + row_id // 16, 1.0, 0.0).astype(BF16)

    loads[0].wait()
    for load in loads[3:]:
        load.start()
    for c in range(8):
        part = nn_dot(gather, hid_v[c * LANE:(c + 1) * LANE, :]).astype(BF16)
        for r in range(8):
            xp[r * LANE + c * 16:r * LANE + (c + 1) * 16, :] = part[r * 16:(r + 1) * 16, :]

    low = lax.broadcasted_iota(jnp.int32, (HALF, LANE), 1) < DIM

    def place(dst, h, half, value):
        for j in range(4):
            pos = ORDER.index((half * 4 + j - h) % 8)
            dst[h, pos * LANE:(pos + 1) * LANE, :] = value[j * LANE:(j + 1) * LANE, :]

    def place_kv(h, half, kp, vp):
        vp = pltpu.roll(vp, DIM, 1)
        place(own, h, half, jnp.where(low, kp, vp).astype(BF16))
        place(own, h + 1, half, jnp.where(low, vp, kp).astype(BF16))

    def project_pair(a):
        at = slice(a * LANE, (a + 1) * LANE)
        both = jnp.concatenate([wk_v[:, at], wv_v[:, at]], axis=1)
        for half in range(2):
            got = nn_dot(xp[half * HALF:(half + 1) * HALF, :], both)
            place_kv(2 * a, half, got[:, 0:LANE], got[:, LANE:TILE])

    def project_kv(cols):
        for half in range(2):
            rows = xp[half * HALF:(half + 1) * HALF, :]
            key = nn_dot(rows, wk_v[:, cols * TILE:(cols + 1) * TILE])
            val = nn_dot(rows, wv_v[:, cols * TILE:(cols + 1) * TILE])
            for a in range(2):
                at = slice(a * LANE, (a + 1) * LANE)
                place_kv(4 * cols + 2 * a, half, key[:, at], val[:, at])

    def project_q(cols):
        for half in range(2):
            qry = nn_dot(xp[half * HALF:(half + 1) * HALF, :], wq_v[:, cols * TILE:(cols + 1) * TILE]) * 0.125
            for a in range(2):
                h = 4 * cols + 2 * a
                qp = qry[:, a * LANE:(a + 1) * LANE]
                place(q_s, h, half, jnp.where(low, qp, 0.0).astype(BF16))
                place(q_s, h + 1, half, jnp.where(low, 0.0, qp).astype(BF16))

    loads[1].wait()
    loads[2].wait()
    project_pair(0)
    pl.semaphore_wait(barrier, 5)
    for h in range(2):
        start(h, 0, 1, 2, 4, 8)
    project_pair(1)
    for h in range(2, 4):
        start(h, 0, 1)
    project_kv(1)
    for h in range(4, HEADS):
        start(h, 0, 1)
    loads[4].wait()
    send_w = pltpu.make_async_remote_copy(
        wo_v.at[:, pl.ds(pl.multiple_of((1 - tp) * HALF, HALF), HALF)], wo_x, osend.at[4], orecv.at[4],
        device_id={'tp': 1 - tp}, device_id_type=MESH)
    send_w.start()
    loads[3].wait()
    project_q(0)
    project_q(1)
    o_t[...] = jnp.zeros_like(o_t)

    def keys(branch, h):
        if branch == 0:
            parts = [own[h], r1[h]]
        elif branch == 1:
            parts = [own[h, 0:HALF, :], r1[h, 0:HALF, :], r2[h]]
        elif branch == 2:
            parts = [own[h, 0:TILE, :], r1[h, 0:TILE, :], r2[h, 0:TILE, :], r2[h, HALF:768, :], r3[h]]
        else:
            parts = [own[h, 0:LANE, :], r1[h, 0:LANE, :], r2[h, 0:LANE, :], r2[h, HALF:640, :]]
            parts += [r3[h, c * TILE:c * TILE + LANE, :] for c in range(4)] + [r4[h]]
        return jnp.concatenate(parts, axis=0)

    def logits(unit, slot):
        branch, h, first, rows = unit
        s = nt_dot(keys(branch, h), q_s[h, first:first + rows, :])
        S[slot][:, 0:rows] = s
        M[slot][:, 0:rows] = jnp.broadcast_to(jnp.max(s, axis=0, keepdims=True), (SUB, rows))

    def soften(unit, slot):
        rows = unit[3]
        m = M[slot][0:1, 0:rows]
        total = jnp.zeros((1, rows), F32)
        for c in range(KEYS // HALF):
            at = slice(c * HALF, (c + 1) * HALF)
            e = jnp.exp(S[slot][at, 0:rows] - m)
            PR[slot][at, 0:rows] = e.astype(BF16)
            total = total + jnp.sum(e, axis=0, keepdims=True)
        T[slot][:, 0:rows] = jnp.broadcast_to(m, (SUB, rows))
        L[slot][:, 0:rows] = jnp.broadcast_to(total, (SUB, rows))

    def gain(unit, slot):
        branch, h, first, rows = unit
        got = tn_dot(keys(branch, h), PR[slot][:, 0:rows])
        total = L[slot][:, 0:rows]
        at = slice(first, first + rows)
        score = T[slot][:, 0:rows] + bias[branch, tp * HEADS + h]
        if branch == 0:
            num[h % 4, :, at] = got
            den[h % 4, :, at] = total
            top[h % 4, :, at] = score
        else:
            old = top[h % 4, :, at]
            new = jnp.maximum(old, score)
            keep = jnp.exp(old - new)
            take = jnp.exp(score - new)
            num[h % 4, :, at] = num[h % 4, :, at] * keep[0:1, :] + got * take[0:1, :]
            den[h % 4, :, at] = den[h % 4, :, at] * keep + total * take
            top[h % 4, :, at] = new

    def send_o(a):
        return pltpu.make_async_remote_copy(o_own.at[a], o_oth.at[a], osend.at[a], orecv.at[a], device_id={'tp': 1 - tp}, device_id_type=MESH)

    def finish(h):
        a, odd = h // 2, h % 2
        have = pl.ds(pl.multiple_of((1 - odd) * DIM, DIM), DIM)
        want = pl.ds(pl.multiple_of(odd * DIM, DIM), DIM)
        for pos in range(8):
            at = slice(pos * LANE, (pos + 1) * LANE)
            to = pl.ds(pl.multiple_of(((ORDER[pos] + h) % 8) * LANE, LANE), LANE)
            o_t[a, want, to] = num[h % 4, have, at] / den[h % 4, 0:1, at]
        for r in range(8):
            at = slice(r * LANE, (r + 1) * LANE)
            o_own[a, at, :] = o_t[a, :, at].T.astype(BF16)

    def unit_of(u, h):
        branch, shift, first, rows = UNITS[u]
        return branch, h + shift, first, rows

    def push(flight, unit):
        slot = (flight[-1][1] + 1) % SLOTS if flight else 0
        pl.delay(1)
        logits(unit, slot)
        if flight:
            soften(*flight[-1])
            gain(*flight[-1])
        return [(unit, slot)], flight[-1][0] if flight else None

    def run(flight, h, *which):
        for u in which:
            flight, done = push(flight, unit_of(u, h))
            if done is not None and done[0] == 3:
                finish(done[1])
        return flight

    event1(0)
    event2(0)
    arrive(0, 1)
    flight = run([], 0, 0)
    event2(1)
    flight = run(flight, 0, 1, 2, 3)
    event3(0)
    event1(1)
    event4(0, 0, 1, 2)
    flight = run(flight, 0, 5, 6)

    def guard(condition, action):
        if not isinstance(condition, bool):
            pl.when(condition)(action)
        elif condition:
            action()

    def pass_of(h, flight):
        arrive(h, 1)
        flight = run(flight, h, 0)
        guard(h + 1 < HEADS, lambda: event2(h + 1))
        guard((h >= 3) & (h % 2 == 1), lambda: send_o((h - 3) // 2).start())
        flight = run(flight, h, 1)
        event4(h - 1, 3)
        flight = run(flight, h, 2, 3, 4)
        event3(h)
        guard(h + 1 < HEADS, lambda: event1(h + 1))
        event4(h, 0, 1, 2)
        flight = run(flight, h, 5, 6)
        arrive_all(h - 1)
        return run(flight, h, 7)

    flight = pass_of(1, flight)

    def body(h, carry):
        left = pass_of(h, [(unit_of(7, h - 1), flight[0][1])])
        assert left[0][1] == flight[0][1]
        return carry

    lax.fori_loop(2, HEADS, body, 0)
    flight = [(unit_of(7, HEADS - 1), flight[0][1])]
    event4(HEADS - 1, 3)
    flight = run(flight, HEADS, 4)
    arrive_all(HEADS - 1)
    flight = run(flight, HEADS, 7)
    soften(*flight[0])
    gain(*flight[0])
    finish(HEADS - 1)
    send_o(3).start()

    mine = pl.ds(pl.multiple_of(tp * HALF, HALF), HALF)

    def heads_of(ref, half):
        return jnp.concatenate([ref[a, half * HALF:(half + 1) * HALF, :] for a in range(4)], axis=1)

    w_mine = wo_v[:, mine]
    for half in range(2):
        part_o[half * HALF:(half + 1) * HALF, :] = nn_dot(heads_of(o_own, half), w_mine)
    send_w.wait()
    for a in range(4):
        send_o(a).wait()
    w_other = wo_x[...]
    for half in range(2):
        at = slice(half * HALF, (half + 1) * HALF)
        out[at, :] = (part_o[at, :] + nn_dot(heads_of(o_oth, half), w_other)).astype(BF16)
    for level in range(4):
        sent(level)


def restore(outp, out):
    row_id = lax.broadcasted_iota(jnp.int32, (LANE, LANE), 0)
    col_id = lax.broadcasted_iota(jnp.int32, (LANE, LANE), 1)
    spread = jnp.where(row_id == 8 * (col_id % 16) + col_id // 16, 1.0, 0.0).astype(BF16)
    for c in range(8):
        part = jnp.concatenate([outp[r * LANE + c * 16:r * LANE + (c + 1) * 16, :] for r in range(8)], axis=0)
        out[c * LANE:(c + 1) * LANE, :] = nn_dot(spread, part).astype(BF16)


def solution(mesh):
    def device_fn(hidden, w_query, w_key, w_value, w_out, branch_bias):
        kv = pltpu.VMEM((HEADS, ROWS, LANE), BF16)
        permuted = pl.pallas_call(
            kernel,
            out_shape=jax.ShapeDtypeStruct((ROWS, HALF), BF16),
            in_specs=[pl.BlockSpec(memory_space=pl.ANY)] * 5 + [pl.BlockSpec(memory_space=pltpu.SMEM)],
            out_specs=pl.BlockSpec(memory_space=pltpu.VMEM),
            scratch_shapes=[
                pltpu.VMEM((ROWS, 1024), BF16),
                pltpu.VMEM((1024, HALF), BF16), pltpu.VMEM((1024, HALF), BF16), pltpu.VMEM((1024, HALF), BF16),
                pltpu.VMEM((HALF, 1024), BF16), pltpu.VMEM((HALF, HALF), BF16),
                pltpu.VMEM((ROWS, 1024), BF16),
                kv, kv, kv, kv, kv, kv,
                *[pltpu.VMEM((KEYS, TILE), F32)] * SLOTS, *[pltpu.VMEM((KEYS, TILE), BF16)] * SLOTS,
                *[pltpu.VMEM((SUB, TILE), F32)] * (3 * SLOTS),
                pltpu.VMEM((4, LANE, ROWS), F32), pltpu.VMEM((4, SUB, ROWS), F32), pltpu.VMEM((4, SUB, ROWS), F32), pltpu.VMEM((4, LANE, ROWS), F32),
                pltpu.VMEM((4, ROWS, LANE), BF16), pltpu.VMEM((4, ROWS, LANE), BF16),
                pltpu.VMEM((ROWS, HALF), F32),
                pltpu.SemaphoreType.DMA((5,)),
                pltpu.SemaphoreType.DMA((4,)), pltpu.SemaphoreType.DMA((HEADS, 9)),
                pltpu.SemaphoreType.DMA((5,)), pltpu.SemaphoreType.DMA((5,)),
            ],
            compiler_params=pltpu.CompilerParams(collective_id=0, has_side_effects=True, vmem_limit_bytes=62 * 1024 * 1024),
            name='dilated',
        )(hidden, w_query, w_key, w_value, w_out, branch_bias)
        return pl.pallas_call(
            restore,
            out_shape=jax.ShapeDtypeStruct((ROWS, HALF), BF16),
            in_specs=[pl.BlockSpec(memory_space=pltpu.VMEM)],
            out_specs=pl.BlockSpec(memory_space=pltpu.VMEM),
            name='restore',
        )(permuted)

    return jax.shard_map(device_fn, mesh=mesh, in_specs=(P(('dp', 'sp'), None), P(None, 'tp'), P(None, 'tp'), P(None, 'tp'), P('tp', None), P(None, None)), out_specs=P(('dp', 'sp'), 'tp'), check_vma=False)
```
